256 devices in a mesh: seq: 64 (over y, x_lo, z), dp: 4 (over x_hi, core).
Axes of the slice: x: 4 (x_hi: 2, x_lo: 2; x = x_hi * 2 + x_lo), y: 4, z: 8, core: 2. Of those that a mesh axis runs over, the one named last changes fastest.
Arguments:
- queries: bfloat16 [4, 16384, 2048], P('dp', 'seq'), may hold values from -12 to 12
- keys: bfloat16 [4, 16384, 1024], P('dp', 'seq'), may hold values from -6 to 6
- values: bfloat16 [4, 16384, 1024], P('dp', 'seq'), may hold values from -6 to 6
- out_grad: bfloat16 [4, 16384, 1792], P('dp', 'seq'), may hold values from -6 to 6
- out_weight: bfloat16 [2048, 1792], P('seq'), may hold values from -0.125 to 0.125
- seq_len: int32 [4], P('dp'), may hold values from 4096 to 16384, as said below
Outputs:
- query_grad: bfloat16 [4, 16384, 2048], P('dp', 'seq')
- key_grad: bfloat16 [4, 16384, 1024], P('dp', 'seq')
- value_grad: bfloat16 [4, 16384, 1024], P('dp', 'seq')
- weight_grad: float32 [2048, 1792], P('seq')
- grad_rms: float32 [], replicated
The draws below stay inside these ranges and needn't reach their ends.
Inputs may be any that keep to these rules, and one draw needn't show every extreme that they name: `seq_len`: at least one sequence has the full length 16384.
All inputs are finite; a program needn't handle non-finite values.
Results may differ from the reference program's by a relative error of at most 0.014.
Values may be sent and summed in bfloat16 or wider, within the bound.
No kernel may reach another device: no remote copies, remote signals or barrier semaphores. Data moves between devices by JAX's collectives and lax.ppermute only.
A program may use at most 128 MiB of HBM per device.

```python
import jax
import jax.numpy as jnp
from jax import lax

HEADS = 8
KV_HEADS = 4
HEAD_DIM = 256
D_OUT = 1792
WINDOW = 512
TOK_DEV = 256
SEQ = 16384
N_SEQ = 64
N_DP = 4


def draw_seq_len(key, part):
    total = TOK_DEV * N_SEQ
    lengths = jax.random.randint(jax.random.fold_in(key, 11), (N_DP,), total // 4, total + 1, dtype=jnp.int32)
    chosen = jax.random.randint(jax.random.fold_in(key, 12), (), 0, N_DP, dtype=jnp.int32)
    places = jnp.arange(N_DP, dtype=jnp.int32)
    return jnp.where(places == chosen, jnp.int32(total), lengths).astype(jnp.int32)


def level_of(rng, extent, cuts, least, top_value):
    loudness, own = 1.0, jax.random.fold_in(rng, 6)
    for axis_at, shards_of in cuts:
        draws = jnp.exp(jax.random.uniform(jax.random.fold_in(own, axis_at), (shards_of,), jnp.float32, least / len(cuts), top_value / len(cuts)))
        loudness = loudness * jnp.repeat(draws, extent[axis_at] // shards_of).reshape([-1 if axis == axis_at else 1 for axis in range(len(extent))])
    return loudness


def scatter_about(stream_key, dims, width, most, split=(), kind=jnp.bfloat16):
    values = jax.random.normal(stream_key, dims, jnp.float32) * width
    if len(split) > 0:
        values = level_of(stream_key, dims, split, -0.22, 0.18) * values
    return jnp.clip(values, min=-most, max=most).astype(kind)


def setup_inputs(seed: int = 0) -> dict:
    arg_keys = jax.random.split(jax.random.key(seed), 7)
    queries = scatter_about(arg_keys[0], (N_DP, SEQ, HEADS * HEAD_DIM), 2.0, 12.0, ((0, 4), (1, 64)))
    keys = scatter_about(arg_keys[1], (N_DP, SEQ, KV_HEADS * HEAD_DIM), 1.0, 6.0, ((0, 4), (1, 64)))
    values = scatter_about(arg_keys[2], (N_DP, SEQ, KV_HEADS * HEAD_DIM), 1.0, 6.0, ((0, 4), (1, 64)))
    out_grad = scatter_about(arg_keys[3], (N_DP, SEQ, D_OUT), 1.0, 6.0, ((0, 4), (1, 64)))
    out_weight = scatter_about(arg_keys[4], (HEADS * HEAD_DIM, D_OUT), (HEADS * HEAD_DIM) ** -0.5, 0.125, ((0, 64),))
    seq_len = draw_seq_len(jax.random.fold_in(arg_keys[6], 71), 0)
    return {"queries": queries, "keys": keys, "values": values, "out_grad": out_grad, "out_weight": out_weight, "seq_len": seq_len}


SCALE = 0.0625
CAP = 50.0

def band_block(q_rows, k_rows, v_rows, g_rows, q_pos, k_pos):
    count = q_rows.shape[0]
    span = k_rows.shape[0]
    group = HEADS // KV_HEADS
    qh = q_rows.astype(jnp.float32).reshape(count, KV_HEADS, group, HEAD_DIM)
    kh = k_rows.astype(jnp.float32).reshape(span, KV_HEADS, HEAD_DIM)
    vh = v_rows.astype(jnp.float32).reshape(span, KV_HEADS, HEAD_DIM)
    gh = g_rows.astype(jnp.float32).reshape(count, KV_HEADS, group, HEAD_DIM)
    raw = jnp.einsum('tkgd,jkd->kgtj', qh, kh) * SCALE
    capped = CAP * jnp.tanh(raw / CAP)
    allowed = (k_pos[None, :] >= 0) & (k_pos[None, :] <= q_pos[:, None]) & (k_pos[None, :] > q_pos[:, None] - WINDOW)
    expo = jnp.where(allowed, jnp.exp(capped), jnp.zeros((), jnp.float32))
    probs = expo / lax.optimization_barrier(jnp.sum(expo, axis=-1, keepdims=True))
    probs_b = probs.astype(jnp.bfloat16)
    attn = jnp.einsum('kgtj,jkd->tkgd', probs_b.astype(jnp.float32), vh).astype(jnp.bfloat16)
    delta = jnp.einsum('tkgd,tkgd->kgt', gh, attn.astype(jnp.float32))[..., None]
    dprob = jnp.einsum('tkgd,jkd->kgtj', gh, vh)
    dscore = (probs * (dprob - delta) * (1.0 - (capped / CAP) ** 2) * SCALE).astype(jnp.bfloat16)
    dscore32 = dscore.astype(jnp.float32)
    dq = jnp.einsum('kgtj,jkd->tkgd', dscore32, kh).reshape(count, -1)
    dk = jnp.einsum('kgtj,tkgd->jkd', dscore32, qh).reshape(span, -1)
    dv = jnp.einsum('kgtj,tkgd->jkd', probs_b.astype(jnp.float32), gh).reshape(span, -1)
    return (dq, dk, dv, attn.reshape(count, -1))

def reference(queries, keys, values, out_grad, out_weight, seq_len):
    seq = TOK_DEV * N_SEQ
    reach = (WINDOW + TOK_DEV - 2) // TOK_DEV
    lead = reach * TOK_DEV
    span = lead + TOK_DEV
    kv_width = KV_HEADS * HEAD_DIM
    q_list = []
    k_list = []
    v_list = []
    weight_raw = jnp.zeros((HEADS * HEAD_DIM, D_OUT), jnp.float32)
    count = jnp.zeros((), jnp.int32)
    for rep in range(N_DP):
        length = seq_len[rep]
        positions = jnp.arange(seq, dtype=jnp.int32)
        valid = positions < length
        masked = jnp.where(valid[:, None], out_grad[rep], jnp.zeros((), jnp.bfloat16))
        grad_attn = jnp.dot(masked, out_weight.T, preferred_element_type=jnp.float32).astype(jnp.bfloat16)
        blank = jnp.zeros((lead, kv_width), jnp.bfloat16)
        key_pad = jnp.concatenate([blank, keys[rep]], 0)
        val_pad = jnp.concatenate([blank, values[rep]], 0)
        rep_queries = queries[rep]

        def step(carry, block):
            dk_pad, dv_pad = carry
            first = (block * TOK_DEV).astype(jnp.int32)
            q_rows = lax.dynamic_slice_in_dim(rep_queries, first, TOK_DEV, 0)
            g_rows = lax.dynamic_slice_in_dim(grad_attn, first, TOK_DEV, 0)
            k_rows = lax.dynamic_slice_in_dim(key_pad, first, span, 0)
            v_rows = lax.dynamic_slice_in_dim(val_pad, first, span, 0)
            q_pos = first + jnp.arange(TOK_DEV, dtype=jnp.int32)
            k_pos = first - lead + jnp.arange(span, dtype=jnp.int32)
            dq, dk, dv, attn = band_block(q_rows, k_rows, v_rows, g_rows, q_pos, k_pos)
            dk_pad = lax.dynamic_update_slice_in_dim(dk_pad, lax.dynamic_slice_in_dim(dk_pad, first, span, 0) + dk, first, 0)
            dv_pad = lax.dynamic_update_slice_in_dim(dv_pad, lax.dynamic_slice_in_dim(dv_pad, first, span, 0) + dv, first, 0)
            return ((dk_pad, dv_pad), (dq, attn))
        init = (jnp.zeros((seq + lead, kv_width), jnp.float32), jnp.zeros((seq + lead, kv_width), jnp.float32))
        (dk_pad, dv_pad), (dq_blocks, attn_blocks) = lax.scan(step, init, jnp.arange(N_SEQ, dtype=jnp.int32))
        q_list.append(dq_blocks.reshape(seq, -1))
        k_list.append(dk_pad[lead:])
        v_list.append(dv_pad[lead:])
        attn_full = attn_blocks.reshape(seq, -1)
        weight_raw = weight_raw + jnp.dot(attn_full.T, masked, preferred_element_type=jnp.float32)
        count = count + jnp.sum(valid.astype(jnp.int32))
    total = count.astype(jnp.float32)
    act_scale = N_DP * seq / total
    weight_scale = lax.rsqrt(total)
    dq_all = jnp.stack(q_list) * act_scale
    dk_all = jnp.stack(k_list) * act_scale
    dv_all = jnp.stack(v_list) * act_scale
    weight_grad = weight_raw * weight_scale
    squares = jnp.sum(dq_all * dq_all) + jnp.sum(dk_all * dk_all) + jnp.sum(dv_all * dv_all) + jnp.sum(weight_grad * weight_grad)
    entries = N_DP * seq * (HEADS + 2 * KV_HEADS) * HEAD_DIM + HEADS * HEAD_DIM * D_OUT
    grad_rms = jnp.sqrt(squares / entries)
    return (dq_all.astype(jnp.bfloat16), dk_all.astype(jnp.bfloat16), dv_all.astype(jnp.bfloat16), weight_grad, grad_rms)
```

```python
import functools
import math

import jax
import jax.numpy as jnp
from jax import lax
from jax.experimental import pallas as pl
from jax.experimental.pallas import tpu as pltpu
from jax.sharding import Mesh
from jax.sharding import PartitionSpec as P

HEADS = 8
KV_HEADS = 4
GROUP = HEADS // KV_HEADS
HEAD_DIM = 256
D_OUT = 1792
HALF = D_OUT // 2
WINDOW = 512
TOK_DEV = 256
WIDTH = HEADS * HEAD_DIM
SEQ = ("seq_0", "seq_1", "seq_2")
DP = ("dp_0", "dp_1")
X_AXES = ("seq_1", "dp_0")
SCALE = 0.0625
CAP = 50.0
EXP_MUL = CAP * math.log2(math.e)
BF16 = jnp.bfloat16
F32 = jnp.float32


def shifted(value, steps):
    count = lax.axis_size(SEQ)
    initial, last = (max(0, -steps), min(count, count - steps))
    return lax.ppermute(value, SEQ, [(source, source + steps) for source in range(initial, last)])


def ring(value, axis, steps):
    count = lax.axis_size(axis)
    return lax.ppermute(value, axis, [(s, (s + steps) % count) for s in range(count)])


def ring_x(value, steps):
    at = lambda x: (x % 2) * 2 + x // 2
    return lax.ppermute(value, X_AXES, [(at(s), at((s + steps) % 4)) for s in range(4)])


def swap(value, axis):
    return lax.ppermute(value, axis, [(0, 1), (1, 0)])


def for_each(value, axis):
    size = lax.axis_size(axis)
    return lax.all_to_all(
        jnp.broadcast_to(value[None], (size, *value.shape)), axis, 0, 0, tiled=True
    )


def dot(a, b, dims):
    return lax.dot_general(a, b, (dims, ((), ())), preferred_element_type=F32)


NT = ((1,), (1,))
NN = ((1,), (0,))
TN = ((0,), (0,))


def squashed(k, q, allowed):
    t = jnp.tanh(dot(k, q, NT) * (SCALE / CAP))
    e = jnp.exp2(t * EXP_MUL)
    if allowed is not None:
        e = jnp.where(allowed, e, 0.0)
    return t, e


def masks(index):
    shape = (TOK_DEV, GROUP * TOK_DEV)
    key = lax.broadcasted_iota(jnp.int32, shape, 0)
    query = lax.broadcasted_iota(jnp.int32, shape, 1) % TOK_DEV
    far = jnp.where(index >= 2, 0, 4 * TOK_DEV)
    near = jnp.where(index >= 1, -1, 4 * TOK_DEV)
    return (key > query + far, key > near, key <= query)


def two_heads(q_ref):
    return jnp.concatenate([q_ref[:, h * HEAD_DIM : (h + 1) * HEAD_DIM] for h in range(GROUP)], 0)


def forward_kernel(at_ref, q_ref, k0_ref, v0_ref, h1_ref, h2_ref, attn_ref):
    q = two_heads(q_ref)
    allowed = masks(at_ref[0])
    keys = (h2_ref[:TOK_DEV], h1_ref[:TOK_DEV], k0_ref[...])
    vals = (h2_ref[TOK_DEV:], h1_ref[TOK_DEV:], v0_ref[...])
    parts = [squashed(k, q, a)[1] for k, a in zip(keys, allowed)]
    total = sum(jnp.sum(e, axis=0, keepdims=True) for e in parts)
    inverse = 1.0 / total
    out = None
    for e, v in zip(parts, vals):
        piece = dot(v, (e * inverse).astype(BF16), TN)
        out = piece if out is None else out + piece
    out = out.astype(BF16)
    for h in range(GROUP):
        attn_ref[h * HEAD_DIM : (h + 1) * HEAD_DIM, :] = out[:, h * TOK_DEV : (h + 1) * TOK_DEV]


def backward_kernel(
    at_ref, scale_ref, q_ref, k0_ref, v0_ref, h1_ref, h2_ref, attn_ref, m_own_ref, m_oth_ref,
    wa_ref, wc_ref, wbl_ref, wbh_ref, wdl_ref, wdh_ref,
    dq_ref, d0_ref, d1_ref, d2_ref, sq_ref, g_ref,
):
    act_scale = scale_ref[0]
    own = pl.multiple_of(at_ref[2] * TOK_DEV, TOK_DEV)
    oth = pl.multiple_of((1 - at_ref[2]) * TOK_DEV, TOK_DEV)
    m_own = m_own_ref[...]
    m_oth = m_oth_ref[...]
    half = HEAD_DIM // 2
    g_ref[:, pl.ds(own, TOK_DEV)] = (
        dot(wa_ref[0], m_own, NT) + dot(wc_ref[0], m_oth, NT)
    ).astype(BF16)
    g_ref[:half, pl.ds(oth, TOK_DEV)] = (
        dot(wbl_ref[0], m_own, NT) + dot(wdl_ref[0], m_oth, NT)
    ).astype(BF16)
    g_ref[half:, pl.ds(oth, TOK_DEV)] = (
        dot(wbh_ref[0], m_own, NT) + dot(wdh_ref[0], m_oth, NT)
    ).astype(BF16)
    g = g_ref[...]
    q = two_heads(q_ref)
    attn = jnp.concatenate(
        [attn_ref[h * HEAD_DIM : (h + 1) * HEAD_DIM, :] for h in range(GROUP)], 1
    )
    delta = jnp.sum(g.astype(F32) * attn.astype(F32), axis=0, keepdims=True)
    allowed = masks(at_ref[0])
    keys = (h2_ref[:TOK_DEV], h1_ref[:TOK_DEV], k0_ref[...])
    vals = (h2_ref[TOK_DEV:], h1_ref[TOK_DEV:], v0_ref[...])
    parts = [squashed(k, q, a) for k, a in zip(keys, allowed)]
    total = sum(jnp.sum(e, axis=0, keepdims=True) for _, e in parts)
    inverse = 1.0 / total
    dq = None
    for (t, e), k, v, out in zip(parts, keys, vals, (d2_ref, d1_ref, d0_ref)):
        probs = e * inverse
        dprob = dot(v, g, NN)
        dscore = (probs * (dprob - delta) * (1.0 - t * t)).astype(BF16)
        piece = dot(k, dscore, TN)
        dq = piece if dq is None else dq + piece
        dk = dot(dscore, q, NN) * (SCALE * act_scale)
        dv = dot(probs.astype(BF16), g, NT) * act_scale
        out[:TOK_DEV] = dk.astype(out.dtype)
        out[TOK_DEV:] = dv.astype(out.dtype)
    dq = dq * (SCALE * act_scale)
    sq_ref[...] = jnp.broadcast_to(jnp.sum(dq * dq), sq_ref.shape)
    for h in range(GROUP):
        dq_ref[:, h * HEAD_DIM : (h + 1) * HEAD_DIM] = dq[
            :, h * TOK_DEV : (h + 1) * TOK_DEV
        ].T.astype(BF16)


def weight_kernel(at_ref, a_own_ref, a_oth_ref, m0_ref, m1_ref, m3_ref, m2a_ref, m2b_ref, out_ref):
    acc = None
    for back, (own, oth) in enumerate(
        (
            (m0_ref[:TOK_DEV], m0_ref[TOK_DEV:]),
            (m1_ref[:TOK_DEV], m1_ref[TOK_DEV:]),
            (m2a_ref[...], m2b_ref[...]),
            (m3_ref[:TOK_DEV], m3_ref[TOK_DEV:]),
        )
    ):
        place = (at_ref[1] + 4 - back) % 4
        both = dot(a_own_ref[place], own, NN) + dot(a_oth_ref[place], oth, NN)
        acc = both if acc is None else acc + both
    out_ref[...] = (
        acc.reshape(16, 2, 16, HALF).transpose(1, 0, 2, 3).reshape(512, HALF).astype(BF16)
    )


def columns(block, at):
    return pl.BlockSpec((block, at[1]), lambda h, *_: (0, h))


def forward(where, q, k, v, h1, h2):
    d = HEAD_DIM
    return pl.pallas_call(
        forward_kernel,
        grid_spec=pltpu.PrefetchScalarGridSpec(
            num_scalar_prefetch=1,
            grid=(KV_HEADS,),
            in_specs=[
                pl.BlockSpec((TOK_DEV, GROUP * d), lambda h, *_: (0, h)),
                pl.BlockSpec((TOK_DEV, d), lambda h, *_: (0, h)),
                pl.BlockSpec((TOK_DEV, d), lambda h, *_: (0, h)),
                pl.BlockSpec((2 * TOK_DEV, d), lambda h, *_: (0, h)),
                pl.BlockSpec((2 * TOK_DEV, d), lambda h, *_: (0, h)),
            ],
            out_specs=pl.BlockSpec((GROUP * d, TOK_DEV), lambda h, *_: (h, 0)),
        ),
        out_shape=jax.ShapeDtypeStruct((WIDTH, TOK_DEV), BF16),
        cost_estimate=pl.CostEstimate(
            flops=2 * 2 * HEADS * 768 * 256 * 256, transcendentals=2 * HEADS * 768 * 256,
            bytes_accessed=5 << 20,
        ),
        name="attention_forward",
    )(where, q, k, v, h1, h2)


def backward(where, scale, q, k, v, h1, h2, attn, m_own, m_oth, weights):
    d = HEAD_DIM
    full = lambda h, *_: (0, 0)
    rel = lambda h, at, *_: ((at[1] + 4 - h) % 4, 0, 0)
    kv_out = lambda t: jax.ShapeDtypeStruct((2 * TOK_DEV, KV_HEADS * d), t)
    return pl.pallas_call(
        backward_kernel,
        grid_spec=pltpu.PrefetchScalarGridSpec(
            num_scalar_prefetch=2,
            grid=(KV_HEADS,),
            in_specs=[
                pl.BlockSpec((TOK_DEV, GROUP * d), lambda h, *_: (0, h)),
                pl.BlockSpec((TOK_DEV, d), lambda h, *_: (0, h)),
                pl.BlockSpec((TOK_DEV, d), lambda h, *_: (0, h)),
                pl.BlockSpec((2 * TOK_DEV, d), lambda h, *_: (0, h)),
                pl.BlockSpec((2 * TOK_DEV, d), lambda h, *_: (0, h)),
                pl.BlockSpec((GROUP * d, TOK_DEV), lambda h, *_: (h, 0)),
                pl.BlockSpec((TOK_DEV, HALF), full),
                pl.BlockSpec((TOK_DEV, HALF), full),
                pl.BlockSpec((1, d, HALF), rel),
                pl.BlockSpec((1, d, HALF), rel),
                pl.BlockSpec((1, d // 2, HALF), rel),
                pl.BlockSpec((1, d // 2, HALF), rel),
                pl.BlockSpec((1, d // 2, HALF), rel),
                pl.BlockSpec((1, d // 2, HALF), rel),
            ],
            out_specs=[
                pl.BlockSpec((TOK_DEV, GROUP * d), lambda h, *_: (0, h)),
                pl.BlockSpec((2 * TOK_DEV, d), lambda h, *_: (0, h)),
                pl.BlockSpec((2 * TOK_DEV, d), lambda h, *_: (0, h)),
                pl.BlockSpec((2 * TOK_DEV, d), lambda h, *_: (0, h)),
                pl.BlockSpec((8, 128), lambda h, *_: (h, 0)),
            ],
            scratch_shapes=[pltpu.VMEM((d, GROUP * TOK_DEV), BF16)],
        ),
        out_shape=[
            jax.ShapeDtypeStruct((TOK_DEV, WIDTH), BF16),
            kv_out(F32),
            kv_out(BF16),
            kv_out(BF16),
            jax.ShapeDtypeStruct((8 * KV_HEADS, 128), F32),
        ],
        cost_estimate=pl.CostEstimate(
            flops=2 * 5 * HEADS * 768 * 256 * 256 + 2 * TOK_DEV * WIDTH * D_OUT,
            transcendentals=2 * HEADS * 768 * 256,
            bytes_accessed=18 << 20,
        ),
        name="attention_backward",
    )(where, scale, q, k, v, h1, h2, attn, m_own, m_oth, *weights)


def weight_product(where, a_own, a_oth, m0, m1, m3, m2a, m2b):
    vmem = pl.BlockSpec(memory_space=pltpu.VMEM)
    return pl.pallas_call(
        weight_kernel,
        in_specs=[pl.BlockSpec(memory_space=pltpu.SMEM)] + [vmem] * 7,
        out_specs=vmem,
        out_shape=jax.ShapeDtypeStruct((512, HALF), BF16),
        cost_estimate=pl.CostEstimate(
            flops=2 * 512 * HALF * 2048, transcendentals=0, bytes_accessed=7 << 20
        ),
        name="weight_product",
    )(where, a_own, a_oth, m0, m1, m3, m2a, m2b)


def shards(queries, keys, values, out_grad, out_weight, seq_len):
    q_rows = queries[0]
    k_rows = keys[0]
    v_rows = values[0]
    length = seq_len[0]
    core = lax.axis_index("dp_1")
    x_hi = lax.axis_index("dp_0")
    index = lax.axis_index(SEQ)
    start = index * TOK_DEV
    where = jnp.stack([index, lax.axis_index("seq_0"), lax.axis_index("seq_1")]).astype(jnp.int32)

    kv = jnp.concatenate([k_rows, v_rows], 0)
    h1 = shifted(kv, 1)
    h2 = shifted(h1, 1)

    half_of = lambda a, c: lax.dynamic_slice_in_dim(a, c * HALF, HALF, 1)
    w_z = for_each(half_of(out_weight, core), "seq_2").reshape(HEAD_DIM, HALF)
    w_up = ring(w_z, "seq_0", 1)
    w_down = ring(w_z, "seq_0", -1)
    mid = HEAD_DIM // 2
    w_far = [ring(w_up[:mid], "seq_0", 1), ring(w_down[mid:], "seq_0", -1)]
    wa = jnp.stack([w_z, w_up, jnp.concatenate(w_far, 0), w_down])
    wbl = ring_x(wa[:, :mid], 1)
    wbh = ring_x(wa[:, mid:], -1)
    wc = swap(wa, "dp_1")
    wdl = swap(wbl, "dp_1")
    wdh = swap(wbh, "dp_1")

    valid = (start + jnp.arange(TOK_DEV, dtype=jnp.int32)) < length
    masked = jnp.where(valid[:, None], out_grad[0], jnp.zeros((), BF16))
    m_own = half_of(masked, core)
    m_oth = half_of(masked, 1 - core)
    m0 = jnp.concatenate([m_own, swap(m_oth, "dp_1")], 0)
    m1 = ring(m0, "seq_0", 1)
    m3 = ring(m0, "seq_0", -1)
    m2a = ring(m1[:TOK_DEV], "seq_0", 1)
    m2b = ring(m3[TOK_DEV:], "seq_0", -1)

    slots = TOK_DEV * lax.axis_size(SEQ) * lax.axis_size(DP)
    count = jnp.clip(length, 0, TOK_DEV * lax.axis_size(SEQ)).astype(F32).reshape(1)
    count = count + swap(count, "dp_1")
    count = count + swap(count, "dp_0")
    act_scale = slots / count
    weight_scale = lax.rsqrt(count[0])

    attn = forward(where, q_rows, k_rows, v_rows, h1, h2)
    a_own = lax.all_to_all(attn, "seq_0", 0, 0, tiled=True)
    a_oth = swap(a_own, "dp_1")

    dq, d0, d1, d2, dq_sq = backward(
        where, act_scale, q_rows, k_rows, v_rows, h1, h2, attn, m_own, m_oth,
        (wa, wc, wbl, wbh, wdl, wdh),
    )
    d1 = (d1.astype(F32) + shifted(d2, -1).astype(F32)).astype(BF16)
    dkv = d0 + shifted(d1, -1).astype(F32)
    square = jnp.sum(dkv * dkv) + jnp.sum(dq_sq.reshape(KV_HEADS, 8, 128)[:, 0, 0])
    dkv = dkv.astype(BF16)

    part = weight_product(
        where, a_own.reshape(4, 512, TOK_DEV), a_oth.reshape(4, 512, TOK_DEV), m0, m1, m3, m2a, m2b
    )
    pieces = lax.all_to_all(part, ("dp_0", "seq_1", "seq_2"), 0, 0, tiled=True)
    piece = jnp.sum(pieces.reshape(32, 16, HALF).astype(F32), axis=0) * weight_scale
    square = square + jnp.sum(piece * piece)

    other = swap(piece, "dp_1")
    row = jnp.where(
        core == 0, jnp.concatenate([piece, other], 1), jnp.concatenate([other, piece], 1)
    )
    other = swap(row, "dp_0")
    weight_grad = jnp.where(
        x_hi == 0, jnp.concatenate([row, other], 0), jnp.concatenate([other, row], 0)
    )

    square = jnp.full((8, 128), square, F32)
    square = jnp.sum(for_each(square, ("dp_0", "seq_1", "dp_1"))[:, 0], axis=0)[0]
    square = jnp.full((8, 128), square, F32)
    square = jnp.sum(for_each(square, ("seq_0", "seq_2"))[:, 0], axis=0)[0]
    entries = slots * (HEADS + 2 * KV_HEADS) * HEAD_DIM + WIDTH * D_OUT
    grad_rms = jnp.sqrt(square / entries)
    return (dq[None], dkv[:TOK_DEV][None], dkv[TOK_DEV:][None], weight_grad, grad_rms)


def solution(mesh):
    split = Mesh(mesh.devices.reshape(4, 2, 8, 2, 2), ("seq_0", "seq_1", "seq_2", "dp_0", "dp_1"))
    placed = (
        P(DP, SEQ, None),
        P(DP, SEQ, None),
        P(DP, SEQ, None),
        P(DP, SEQ, None),
        P(SEQ, None),
        P(DP),
    )
    return jax.shard_map(
        shards,
        mesh=split,
        in_specs=placed,
        out_specs=(P(DP, SEQ, None), P(DP, SEQ, None), P(DP, SEQ, None), P(SEQ, None), P()),
        check_vma=False,
    )
```

```python
import math

import jax
import jax.numpy as jnp
from jax import lax
from jax.experimental import pallas as pl
from jax.experimental.pallas import tpu as pltpu
from jax.sharding import Mesh
from jax.sharding import PartitionSpec as P


HEADS = 8
KV_HEADS = 4
GROUP = HEADS // KV_HEADS
HEAD_DIM = 256
D_OUT = 1792
HALF = D_OUT // 2
TOK_DEV = 256
WIDTH = HEADS * HEAD_DIM
SEQ = ("seq_0", "seq_1", "seq_2")
DP = ("dp_0", "dp_1")
X_AXES = ("seq_1", "dp_0")
SCALE = 0.0625
CAP = 50.0
EXP_MUL = CAP * math.log2(math.e)
BF16 = jnp.bfloat16
F32 = jnp.float32


def shifted(value, steps):
    count = lax.axis_size(SEQ)
    initial, last = (max(0, -steps), min(count, count - steps))
    return lax.ppermute(value, SEQ, [(source, source + steps) for source in range(initial, last)])


def ring(value, axis, steps):
    count = lax.axis_size(axis)
    return lax.ppermute(value, axis, [(s, (s + steps) % count) for s in range(count)])


def ring_x(value, steps):
    at = lambda x: (x % 2) * 2 + x // 2
    return lax.ppermute(value, X_AXES, [(at(s), at((s + steps) % 4)) for s in range(4)])


def swap(value, axis):
    return lax.ppermute(value, axis, [(0, 1), (1, 0)])


def for_each(value, axis):
    size = lax.axis_size(axis)
    return lax.all_to_all(
        jnp.broadcast_to(value[None], (size, *value.shape)), axis, 0, 0, tiled=True
    )


def dot(a, b, dims):
    return lax.dot_general(a, b, (dims, ((), ())), preferred_element_type=F32)


NT = ((1,), (1,))
NN = ((1,), (0,))
TN = ((0,), (0,))


def squashed(k, q):
    t = jnp.tanh(dot(k, q, NT) * (SCALE / CAP))
    return t, jnp.exp2(t * EXP_MUL)


def places():
    shape = (TOK_DEV, GROUP * TOK_DEV)
    key = lax.broadcasted_iota(jnp.int32, shape, 0)
    query = lax.broadcasted_iota(jnp.int32, shape, 1) & (TOK_DEV - 1)
    return key, query


def two_heads(q_ref):
    return jnp.concatenate([q_ref[:, h * HEAD_DIM : (h + 1) * HEAD_DIM] for h in range(GROUP)], 0)


def row_sum(e):
    return jnp.sum(e, axis=0, keepdims=True)


def near_kernel(at_ref, q_ref, k0_ref, v0_ref, h1_ref, p_ref, pf_ref, acc_ref, tot_ref):
    q = two_heads(q_ref)
    key, query = places()
    t, e = squashed(h1_ref[:TOK_DEV], q)
    e = e * jnp.where(at_ref[0] >= 1, 1.0, 0.0)
    p1 = e.astype(BF16)
    p_ref[0, :TOK_DEV] = p1
    pf_ref[0, :TOK_DEV] = (e * (1.0 - t * t)).astype(BF16)
    total = row_sum(e)
    t, e = squashed(k0_ref[...], q)
    e = jnp.where(key <= query, e, 0.0)
    p0 = e.astype(BF16)
    p_ref[0, TOK_DEV:] = p0
    pf_ref[0, TOK_DEV:] = (e * (1.0 - t * t)).astype(BF16)
    total = total + row_sum(e)
    acc_ref[0] = dot(h1_ref[TOK_DEV:], p1, TN) + dot(v0_ref[...], p0, TN)
    tot_ref[0] = jnp.broadcast_to(total, tot_ref.shape[1:])


def far_kernel(at_ref, q_ref, h2_ref, acc_ref, tot_ref, p_ref, pf_ref, attn_ref, inv_ref):
    key, query = places()
    t, e = squashed(h2_ref[:TOK_DEV], two_heads(q_ref))
    e = jnp.where(key > query + jnp.where(at_ref[0] >= 2, 0, 4 * TOK_DEV), e, 0.0)
    p = e.astype(BF16)
    p_ref[0] = p
    pf_ref[0] = (e * (1.0 - t * t)).astype(BF16)
    inverse = 1.0 / (tot_ref[0, :1] + row_sum(e))
    inv_ref[0] = jnp.broadcast_to(inverse, inv_ref.shape[1:])
    out = ((acc_ref[0] + dot(h2_ref[TOK_DEV:], p, TN)) * inverse).astype(BF16)
    for h in range(GROUP):
        attn_ref[h * HEAD_DIM : (h + 1) * HEAD_DIM, :] = out[:, h * TOK_DEV : (h + 1) * TOK_DEV]


def terms(k, v, q, p, pf, g, delta):
    dscore = (pf.astype(F32) * (dot(v, g, NN) - delta)).astype(BF16)
    return dot(k, dscore, TN), dot(dscore, q, NN), dot(p, g, NT)


def far_grad_kernel(
    at_ref, scale_ref, q_ref, h2_ref, p_ref, pf_ref, inv_ref, attn_ref, m_own_ref, m_oth_ref,
    wa_ref, wc_ref, wbl_ref, wbh_ref, wdl_ref, wdh_ref,
    d2_ref, g_ref, delta_ref, dq_ref, raw_ref,
):
    act_scale = scale_ref[0]
    own = pl.multiple_of(at_ref[2] * TOK_DEV, TOK_DEV)
    oth = pl.multiple_of((1 - at_ref[2]) * TOK_DEV, TOK_DEV)
    m_own = m_own_ref[...]
    m_oth = m_oth_ref[...]
    half = HEAD_DIM // 2
    raw_ref[:, pl.ds(own, TOK_DEV)] = dot(wa_ref[0], m_own, NT) + dot(wc_ref[0], m_oth, NT)
    raw_ref[:half, pl.ds(oth, TOK_DEV)] = dot(wbl_ref[0], m_own, NT) + dot(wdl_ref[0], m_oth, NT)
    raw_ref[half:, pl.ds(oth, TOK_DEV)] = dot(wbh_ref[0], m_own, NT) + dot(wdh_ref[0], m_oth, NT)
    g = (raw_ref[...] * inv_ref[0, :1]).astype(BF16)
    g_ref[0] = g
    attn = jnp.concatenate(
        [attn_ref[h * HEAD_DIM : (h + 1) * HEAD_DIM, :] for h in range(GROUP)], 1
    )
    delta = row_sum(g.astype(F32) * attn.astype(F32))
    delta_ref[0] = jnp.broadcast_to(delta, delta_ref.shape[1:])
    dq, dk, dv = terms(
        h2_ref[:TOK_DEV], h2_ref[TOK_DEV:], two_heads(q_ref), p_ref[0], pf_ref[0], g, delta
    )
    dq_ref[0] = dq
    d2_ref[:TOK_DEV] = (dk * (SCALE * act_scale)).astype(BF16)
    d2_ref[TOK_DEV:] = (dv * act_scale).astype(BF16)


def near_grad_kernel(
    scale_ref, q_ref, k0_ref, v0_ref, h1_ref, p_ref, pf_ref, g_ref, delta_ref, far_ref,
    dq_ref, d0_ref, d1_ref, sq_ref,
):
    act_scale = scale_ref[0]
    q = two_heads(q_ref)
    g = g_ref[0]
    delta = delta_ref[0, :1]
    dq = far_ref[0]
    for k, v, at, out in (
        (h1_ref[:TOK_DEV], h1_ref[TOK_DEV:], 0, d1_ref),
        (k0_ref[...], v0_ref[...], TOK_DEV, d0_ref),
    ):
        piece, dk, dv = terms(
            k, v, q, p_ref[0, at : at + TOK_DEV], pf_ref[0, at : at + TOK_DEV], g, delta
        )
        dq = dq + piece
        out[:TOK_DEV] = (dk * (SCALE * act_scale)).astype(out.dtype)
        out[TOK_DEV:] = (dv * act_scale).astype(out.dtype)
    dq = dq * (SCALE * act_scale)
    sq_ref[...] = jnp.broadcast_to(jnp.sum(dq * dq), sq_ref.shape)
    for h in range(GROUP):
        dq_ref[:, h * HEAD_DIM : (h + 1) * HEAD_DIM] = dq[
            :, h * TOK_DEV : (h + 1) * TOK_DEV
        ].T.astype(BF16)


def weight_kernel(at_ref, a_own_ref, a_oth_ref, m0_ref, m1_ref, m3_ref, m2a_ref, m2b_ref, out_ref):
    acc = None
    for back, (own, oth) in enumerate(
        (
            (m0_ref[:TOK_DEV], m0_ref[TOK_DEV:]),
            (m1_ref[:TOK_DEV], m1_ref[TOK_DEV:]),
            (m2a_ref[...], m2b_ref[...]),
            (m3_ref[:TOK_DEV], m3_ref[TOK_DEV:]),
        )
    ):
        place = (at_ref[1] + 4 - back) % 4
        both = dot(a_own_ref[place], own, NN) + dot(a_oth_ref[place], oth, NN)
        acc = both if acc is None else acc + both
    acc = acc.reshape(2, 8, 2, 16, HALF)
    for low in range(2):
        for high in range(2):
            away = (2 * high + low + 4 - at_ref[3]) % 4
            out_ref[away] = acc[low, :, high].reshape(128, HALF).astype(BF16)


D = HEAD_DIM
SCORES = GROUP * TOK_DEV
HEAD_COLS = pl.BlockSpec((TOK_DEV, GROUP * D), lambda h, *_: (0, h))
KV_COLS = pl.BlockSpec((TOK_DEV, D), lambda h, *_: (0, h))
BOTH_COLS = pl.BlockSpec((2 * TOK_DEV, D), lambda h, *_: (0, h))
ATTN_ROWS = pl.BlockSpec((GROUP * D, TOK_DEV), lambda h, *_: (h, 0))


def of_head(rows, columns=SCORES):
    return pl.BlockSpec((1, rows, columns), lambda h, *_: (h, 0, 0))


def per_head(rows, dtype):
    return jax.ShapeDtypeStruct((KV_HEADS, rows, SCORES), dtype)


def flat(rows, dtype):
    return jax.ShapeDtypeStruct((rows, KV_HEADS * D), dtype)


def call(kernel, scalars, in_specs, out_specs, out_shape, products, mib, scratch=()):
    return pl.pallas_call(
        kernel,
        grid_spec=pltpu.PrefetchScalarGridSpec(
            num_scalar_prefetch=scalars,
            grid=(KV_HEADS,),
            in_specs=in_specs,
            out_specs=out_specs,
            scratch_shapes=scratch,
        ),
        out_shape=out_shape,
        cost_estimate=pl.CostEstimate(
            flops=products * 2 * HEADS * TOK_DEV**3, transcendentals=0, bytes_accessed=mib << 20
        ),
    )


def near_forward(where, q, k, v, h1):
    return call(
        near_kernel, 1,
        [HEAD_COLS, KV_COLS, KV_COLS, BOTH_COLS],
        [of_head(2 * TOK_DEV), of_head(2 * TOK_DEV), of_head(D), of_head(8)],
        [per_head(2 * TOK_DEV, BF16), per_head(2 * TOK_DEV, BF16), per_head(D, F32),
         per_head(8, F32)],
        4, 9,
    )(where, q, k, v, h1)


def far_forward(where, q, h2, acc, tot):
    return call(
        far_kernel, 1,
        [HEAD_COLS, BOTH_COLS, of_head(D), of_head(8)],
        [of_head(TOK_DEV), of_head(TOK_DEV), ATTN_ROWS, of_head(8)],
        [per_head(TOK_DEV, BF16), per_head(TOK_DEV, BF16),
         jax.ShapeDtypeStruct((WIDTH, TOK_DEV), BF16), per_head(8, F32)],
        2, 7,
    )(where, q, h2, acc, tot)


def far_backward(where, scale, q, h2, p, pf, inv, attn, m_own, m_oth, weights):
    full = pl.BlockSpec((TOK_DEV, HALF), lambda h, *_: (0, 0))
    rel = lambda rows: pl.BlockSpec((1, rows, HALF), lambda h, at, *_: ((at[1] + 4 - h) % 4, 0, 0))
    return call(
        far_grad_kernel, 2,
        [HEAD_COLS, BOTH_COLS, of_head(TOK_DEV), of_head(TOK_DEV), of_head(8), ATTN_ROWS, full,
         full, rel(D), rel(D)] + [rel(D // 2)] * 4,
        [BOTH_COLS, of_head(D), of_head(8), of_head(D)],
        [flat(2 * TOK_DEV, BF16), per_head(D, BF16), per_head(8, F32), per_head(D, F32)],
        4 + 7, 16, [pltpu.VMEM((D, SCORES), F32)],
    )(where, scale, q, h2, p, pf, inv, attn, m_own, m_oth, *weights)


def near_backward(scale, q, k, v, h1, p, pf, g, delta, far):
    return call(
        near_grad_kernel, 1,
        [HEAD_COLS, KV_COLS, KV_COLS, BOTH_COLS, of_head(2 * TOK_DEV), of_head(2 * TOK_DEV),
         of_head(D), of_head(8), of_head(D)],
        [HEAD_COLS, BOTH_COLS, BOTH_COLS, pl.BlockSpec((8, 128), lambda h, *_: (h, 0))],
        [jax.ShapeDtypeStruct((TOK_DEV, WIDTH), BF16), flat(2 * TOK_DEV, F32),
         flat(2 * TOK_DEV, BF16), jax.ShapeDtypeStruct((8 * KV_HEADS, 128), F32)],
        8, 14,
    )(scale, q, k, v, h1, p, pf, g, delta, far)


def weight_product(where, a_own, a_oth, m0, m1, m3, m2a, m2b):
    vmem = pl.BlockSpec(memory_space=pltpu.VMEM)
    return pl.pallas_call(
        weight_kernel,
        in_specs=[pl.BlockSpec(memory_space=pltpu.SMEM)] + [vmem] * 7,
        out_specs=vmem,
        out_shape=jax.ShapeDtypeStruct((4, 128, HALF), BF16),
        cost_estimate=pl.CostEstimate(
            flops=2 * 512 * HALF * 2048, transcendentals=0, bytes_accessed=7 << 20
        ),
        name="weight_product",
    )(where, a_own, a_oth, m0, m1, m3, m2a, m2b)


def all_steps(queries, keys, values, out_grad, out_weight, seq_len):
    q_rows = queries[0]
    k_rows = keys[0]
    v_rows = values[0]
    length = seq_len[0]
    core = lax.axis_index("dp_1")
    x_hi = lax.axis_index("dp_0")
    x_lo = lax.axis_index("seq_1")
    index = lax.axis_index(SEQ)
    start = index * TOK_DEV
    where = jnp.stack([index, lax.axis_index("seq_0"), x_lo, 2 * x_hi + x_lo]).astype(jnp.int32)

    kv = jnp.concatenate([k_rows, v_rows], 0)
    h1 = shifted(kv, 1)
    h2 = shifted(h1, 1)

    slots = TOK_DEV * lax.axis_size(SEQ) * lax.axis_size(DP)
    count = jnp.clip(length, 0, TOK_DEV * lax.axis_size(SEQ)).astype(F32).reshape(1)
    count = count + swap(count, "dp_1")
    count = count + swap(count, "dp_0")
    act_scale = slots / count
    weight_scale = lax.rsqrt(count[0])

    half_of = lambda a, c: lax.dynamic_slice_in_dim(a, c * HALF, HALF, 1)
    valid = (start + jnp.arange(TOK_DEV, dtype=jnp.int32)) < length
    masked = jnp.where(valid[:, None], out_grad[0], jnp.zeros((), BF16))
    m_own = half_of(masked, core)
    m_oth = half_of(masked, 1 - core)
    m0 = jnp.concatenate([m_own, swap(m_oth, "dp_1")], 0)
    m1 = ring(m0, "seq_0", 1)
    m3 = ring(m0, "seq_0", -1)
    m2a = ring(m1[:TOK_DEV], "seq_0", 1)
    m2b = ring(m3[TOK_DEV:], "seq_0", -1)

    w_z = for_each(half_of(out_weight, core), "seq_2").reshape(HEAD_DIM, HALF)
    w_up = ring(w_z, "seq_0", 1)
    w_down = ring(w_z, "seq_0", -1)
    mid = HEAD_DIM // 2
    w_far = [ring(w_up[:mid], "seq_0", 1), ring(w_down[mid:], "seq_0", -1)]
    wa = jnp.stack([w_z, w_up, jnp.concatenate(w_far, 0), w_down])
    wbl = ring_x(wa[:, :mid], 1)
    wbh = ring_x(wa[:, mid:], -1)
    wc = swap(wa, "dp_1")
    wdl = swap(wbl, "dp_1")
    wdh = swap(wbh, "dp_1")

    p, pf, acc, tot = near_forward(where, q_rows, k_rows, v_rows, h1)
    p2, pf2, attn, inv = far_forward(where, q_rows, h2, acc, tot)
    a_own = lax.all_to_all(attn, "seq_0", 0, 0, tiled=True)
    a_oth = swap(a_own, "dp_1")

    d2, g, delta, far = far_backward(
        where, act_scale, q_rows, h2, p2, pf2, inv, attn, m_own, m_oth,
        (wa, wc, wbl, wbh, wdl, wdh),
    )
    r1 = shifted(d2, -1)
    dq, d0, d1, dq_sq = near_backward(
        act_scale, q_rows, k_rows, v_rows, h1, p, pf, g, delta, far
    )
    r2 = shifted((d1.astype(F32) + r1.astype(F32)).astype(BF16), -1)
    dkv = d0 + r2.astype(F32)
    square = jnp.sum(dkv * dkv) + jnp.sum(dq_sq.reshape(KV_HEADS, 8, 128)[:, 0, 0])
    dkv = dkv.astype(BF16)

    part = weight_product(
        where, a_own.reshape(4, 512, TOK_DEV), a_oth.reshape(4, 512, TOK_DEV), m0, m1, m3, m2a, m2b
    )
    part = (
        part[0].astype(F32)
        + ring_x(part[1], 1).astype(F32)
        + ring_x(part[2], 2).astype(F32)
        + ring_x(part[3], -1).astype(F32)
    ).astype(BF16)
    pieces = lax.all_to_all(part, "seq_2", 0, 0, tiled=True)
    piece = jnp.sum(pieces.reshape(8, 16, HALF).astype(F32), axis=0) * weight_scale
    square = square + jnp.sum(piece * piece)

    other = swap(piece, "dp_1")
    row = jnp.where(
        core == 0, jnp.concatenate([piece, other], 1), jnp.concatenate([other, piece], 1)
    )
    other = swap(row, "dp_0")
    weight_grad = jnp.where(
        x_hi == 0, jnp.concatenate([row, other], 0), jnp.concatenate([other, row], 0)
    )

    square = jnp.full((8, 128), square, F32)
    square = for_each(square, ("dp_0", "seq_1", "dp_1"))
    square = jnp.full((8, 128), jnp.sum(square[:, 0], axis=0)[0], F32)
    square = for_each(square, ("seq_0", "seq_2"))
    square = jnp.sum(square[:, 0], axis=0)[0]
    entries = slots * (HEADS + 2 * KV_HEADS) * HEAD_DIM + WIDTH * D_OUT
    grad_rms = jnp.sqrt(square / entries)
    return (dq[None], dkv[:TOK_DEV][None], dkv[TOK_DEV:][None], weight_grad, grad_rms)


def solution(mesh):
    split = Mesh(mesh.devices.reshape(4, 2, 8, 2, 2), ("seq_0", "seq_1", "seq_2", "dp_0", "dp_1"))
    placed = (
        P(DP, SEQ, None),
        P(DP, SEQ, None),
        P(DP, SEQ, None),
        P(DP, SEQ, None),
        P(SEQ, None),
        P(DP),
    )
    return jax.shard_map(
        all_steps,
        mesh=split,
        in_specs=placed,
        out_specs=(P(DP, SEQ, None), P(DP, SEQ, None), P(DP, SEQ, None), P(SEQ, None), P()),
        check_vma=False,
    )
```

```python
import math

import jax
import jax.numpy as jnp
from jax import lax
from jax.experimental import pallas as pl
from jax.experimental.pallas import tpu as pltpu
from jax.sharding import Mesh
from jax.sharding import PartitionSpec as P


HEADS = 8
KV_HEADS = 4
GROUP = HEADS // KV_HEADS
HEAD_DIM = 256
D_OUT = 1792
HALF = D_OUT // 2
TOK_DEV = 256
WIDTH = HEADS * HEAD_DIM
SEQ = ("seq_0", "seq_1", "seq_2")
DP = ("dp_0", "dp_1")
X_AXES = ("seq_1", "dp_0")
SCALE = 0.0625
CAP = 50.0
EXP_MUL = CAP * math.log2(math.e)
BF16 = jnp.bfloat16
F32 = jnp.float32


def shifted(value, steps):
    count = lax.axis_size(SEQ)
    initial, last = (max(0, -steps), min(count, count - steps))
    return lax.ppermute(value, SEQ, [(source, source + steps) for source in range(initial, last)])


def ring(value, axis, steps):
    count = lax.axis_size(axis)
    return lax.ppermute(value, axis, [(s, (s + steps) % count) for s in range(count)])


def ring_x(value, steps):
    at = lambda x: (x % 2) * 2 + x // 2
    return lax.ppermute(value, X_AXES, [(at(s), at((s + steps) % 4)) for s in range(4)])


def across_x(value, steps):
    pairs = []
    depth = lax.axis_size("seq_2")
    for low in range(2):
        for z in range(depth):
            for high in range(2):
                step = steps if z else (1 if low else -1)
                to = (2 * high + low + step) % 4
                pairs.append(
                    ((low * depth + z) * 2 + high, ((to % 2) * depth + z) * 2 + to // 2)
                )
    return lax.ppermute(value, ("seq_1", "seq_2", "dp_0"), pairs)


def swap(value, axis):
    return lax.ppermute(value, axis, [(0, 1), (1, 0)])


def for_each(value, axis):
    size = lax.axis_size(axis)
    return lax.all_to_all(
        jnp.broadcast_to(value[None], (size, *value.shape)), axis, 0, 0, tiled=True
    )


def dot(a, b, dims):
    return lax.dot_general(a, b, (dims, ((), ())), preferred_element_type=F32)


NT = ((1,), (1,))
NN = ((1,), (0,))
TN = ((0,), (0,))


def squashed(k, q):
    t = jnp.tanh(dot(k, q, NT) * (SCALE / CAP))
    return t, jnp.exp2(t * EXP_MUL)


def places():
    shape = (TOK_DEV, GROUP * TOK_DEV)
    key = lax.broadcasted_iota(jnp.int32, shape, 0)
    query = lax.broadcasted_iota(jnp.int32, shape, 1) & (TOK_DEV - 1)
    return key, query


def two_heads(q_ref):
    return jnp.concatenate([q_ref[:, h * HEAD_DIM : (h + 1) * HEAD_DIM] for h in range(GROUP)], 0)


def row_sum(e):
    return jnp.sum(e, axis=0, keepdims=True)


def near_kernel(at_ref, q_ref, k0_ref, v0_ref, h1_ref, p_ref, pf_ref, acc_ref, tot_ref):
    q = two_heads(q_ref)
    key, query = places()
    t, e = squashed(h1_ref[:TOK_DEV], q)
    e = e * jnp.where(at_ref[0] >= 1, 1.0, 0.0)
    p1 = e.astype(BF16)
    p_ref[0, :TOK_DEV] = p1
    pf_ref[0, :TOK_DEV] = (e * (1.0 - t * t)).astype(BF16)
    total = row_sum(e)
    t, e = squashed(k0_ref[...], q)
    e = jnp.where(key <= query, e, 0.0)
    p0 = e.astype(BF16)
    p_ref[0, TOK_DEV:] = p0
    pf_ref[0, TOK_DEV:] = (e * (1.0 - t * t)).astype(BF16)
    total = total + row_sum(e)
    acc_ref[0] = dot(h1_ref[TOK_DEV:], p1, TN) + dot(v0_ref[...], p0, TN)
    tot_ref[0] = jnp.broadcast_to(total, tot_ref.shape[1:])


def far_kernel(at_ref, q_ref, h2_ref, acc_ref, tot_ref, p_ref, pf_ref, attn_ref, inv_ref):
    key, query = places()
    t, e = squashed(h2_ref[:TOK_DEV], two_heads(q_ref))
    e = jnp.where(key > query + jnp.where(at_ref[0] >= 2, 0, 4 * TOK_DEV), e, 0.0)
    p = e.astype(BF16)
    p_ref[0] = p
    pf_ref[0] = (e * (1.0 - t * t)).astype(BF16)
    inverse = 1.0 / (tot_ref[0, :1] + row_sum(e))
    inv_ref[0] = jnp.broadcast_to(inverse, inv_ref.shape[1:])
    out = ((acc_ref[0] + dot(h2_ref[TOK_DEV:], p, TN)) * inverse).astype(BF16)
    for h in range(GROUP):
        attn_ref[0, h * HEAD_DIM : (h + 1) * HEAD_DIM, :] = out[:, h * TOK_DEV : (h + 1) * TOK_DEV]


def score_terms(v, g, delta, pf):
    return (pf.astype(F32) * (dot(v, g, NN) - delta)).astype(BF16)


def far_grad_kernel(
    at_ref, scale_ref, q_ref, h2_ref, p_ref, pf_ref, inv_ref, attn_ref, m_own_ref, m_oth_ref,
    wa_ref, wc_ref, wbl_ref, wbh_ref, wdl_ref, wdh_ref,
    d2_ref, g_ref, delta_ref, ds_ref, raw_ref,
):
    act_scale = scale_ref[0]
    own = pl.multiple_of(at_ref[2] * TOK_DEV, TOK_DEV)
    oth = pl.multiple_of((1 - at_ref[2]) * TOK_DEV, TOK_DEV)
    both = dot(
        jnp.concatenate([wa_ref[0], wbl_ref[0], wbh_ref[0]], 0), m_own_ref[...], NT
    ) + dot(jnp.concatenate([wc_ref[0], wdl_ref[0], wdh_ref[0]], 0), m_oth_ref[...], NT)
    raw_ref[:, pl.ds(own, TOK_DEV)] = both[:HEAD_DIM]
    raw_ref[:, pl.ds(oth, TOK_DEV)] = both[HEAD_DIM:]
    g = (raw_ref[...] * inv_ref[0, :1]).astype(BF16)
    g_ref[0] = g
    attn = jnp.concatenate(
        [attn_ref[0, h * HEAD_DIM : (h + 1) * HEAD_DIM, :] for h in range(GROUP)], 1
    )
    delta = row_sum(g.astype(F32) * attn.astype(F32))
    delta_ref[0] = jnp.broadcast_to(delta, delta_ref.shape[1:])
    dscore = score_terms(h2_ref[TOK_DEV:], g, delta, pf_ref[0])
    ds_ref[0] = dscore
    d2_ref[:TOK_DEV] = (dot(dscore, two_heads(q_ref), NN) * (SCALE * act_scale)).astype(BF16)
    d2_ref[TOK_DEV:] = (dot(p_ref[0], g, NT) * act_scale).astype(BF16)


def near_grad_kernel(
    scale_ref, q_ref, k0_ref, v0_ref, h1_ref, h2_ref, p_ref, pf_ref, g_ref, delta_ref, ds_ref,
    dq_ref, d0_ref, d1_ref, sq_ref,
):
    act_scale = scale_ref[0]
    q = two_heads(q_ref)
    g = g_ref[0]
    delta = delta_ref[0, :1]
    dq = dot(h2_ref[...], ds_ref[0], TN)
    for k, v, at, out in (
        (h1_ref[:TOK_DEV], h1_ref[TOK_DEV:], 0, d1_ref),
        (k0_ref[...], v0_ref[...], TOK_DEV, d0_ref),
    ):
        dscore = score_terms(v, g, delta, pf_ref[0, at : at + TOK_DEV])
        dq = dq + dot(k, dscore, TN)
        out[:TOK_DEV] = (dot(dscore, q, NN) * (SCALE * act_scale)).astype(out.dtype)
        out[TOK_DEV:] = (dot(p_ref[0, at : at + TOK_DEV], g, NT) * act_scale).astype(out.dtype)
    dq = dq * (SCALE * act_scale)
    sq_ref[...] = jnp.broadcast_to(jnp.sum(dq * dq), sq_ref.shape)
    for h in range(GROUP):
        dq_ref[:, h * HEAD_DIM : (h + 1) * HEAD_DIM] = dq[
            :, h * TOK_DEV : (h + 1) * TOK_DEV
        ].T.astype(BF16)


def weight_kernel(at_ref, a_own_ref, a_oth_ref, m0_ref, m1_ref, m3_ref, m2a_ref, m2b_ref, out_ref):
    acc = None
    for back, (own, oth) in enumerate(
        (
            (m0_ref[:TOK_DEV], m0_ref[TOK_DEV:]),
            (m1_ref[:TOK_DEV], m1_ref[TOK_DEV:]),
            (m2a_ref[...], m2b_ref[...]),
            (m3_ref[:TOK_DEV], m3_ref[TOK_DEV:]),
        )
    ):
        both = dot(a_own_ref[back], own, NN) + dot(a_oth_ref[back], oth, NN)
        acc = both if acc is None else acc + both
    acc = acc.reshape(2, 8, 2, 16, HALF)
    for low in range(2):
        for high in range(2):
            away = (2 * high + low + 4 - at_ref[3]) % 4
            out_ref[away] = acc[low, :, high].reshape(128, HALF).astype(BF16)


D = HEAD_DIM
SCORES = GROUP * TOK_DEV
HEAD_COLS = pl.BlockSpec((TOK_DEV, GROUP * D), lambda h, *_: (0, h))
KV_COLS = pl.BlockSpec((TOK_DEV, D), lambda h, *_: (0, h))
BOTH_COLS = pl.BlockSpec((2 * TOK_DEV, D), lambda h, *_: (0, h))
ATTN_ROWS = pl.BlockSpec((1, GROUP * D, TOK_DEV), lambda h, at, *_: ((h + 4 - at[1]) % 4, 0, 0))


def of_head(rows, columns=SCORES):
    return pl.BlockSpec((1, rows, columns), lambda h, *_: (h, 0, 0))


def per_head(rows, dtype):
    return jax.ShapeDtypeStruct((KV_HEADS, rows, SCORES), dtype)


def flat(rows, dtype):
    return jax.ShapeDtypeStruct((rows, KV_HEADS * D), dtype)


def call(kernel, scalars, in_specs, out_specs, out_shape, products, mib, scratch=()):
    return pl.pallas_call(
        kernel,
        grid_spec=pltpu.PrefetchScalarGridSpec(
            num_scalar_prefetch=scalars,
            grid=(KV_HEADS,),
            in_specs=in_specs,
            out_specs=out_specs,
            scratch_shapes=scratch,
        ),
        out_shape=out_shape,
        cost_estimate=pl.CostEstimate(
            flops=products * 2 * HEADS * TOK_DEV**3, transcendentals=0, bytes_accessed=mib << 20
        ),
    )


def near_forward(where, q, k, v, h1):
    return call(
        near_kernel, 1,
        [HEAD_COLS, KV_COLS, KV_COLS, BOTH_COLS],
        [of_head(2 * TOK_DEV), of_head(2 * TOK_DEV), of_head(D), of_head(8)],
        [per_head(2 * TOK_DEV, BF16), per_head(2 * TOK_DEV, BF16), per_head(D, F32),
         per_head(8, F32)],
        4, 9,
    )(where, q, k, v, h1)


def far_forward(where, q, h2, acc, tot):
    return call(
        far_kernel, 1,
        [HEAD_COLS, BOTH_COLS, of_head(D), of_head(8)],
        [of_head(TOK_DEV), of_head(TOK_DEV), ATTN_ROWS, of_head(8)],
        [per_head(TOK_DEV, BF16), per_head(TOK_DEV, BF16),
         jax.ShapeDtypeStruct((KV_HEADS, GROUP * D, TOK_DEV), BF16), per_head(8, F32)],
        2, 7,
    )(where, q, h2, acc, tot)


def far_backward(where, scale, q, h2, p, pf, inv, attn, m_own, m_oth, weights):
    full = pl.BlockSpec((TOK_DEV, HALF), lambda h, *_: (0, 0))
    rel = lambda rows: pl.BlockSpec((1, rows, HALF), lambda h, at, *_: ((at[1] + 4 - h) % 4, 0, 0))
    return call(
        far_grad_kernel, 2,
        [HEAD_COLS, BOTH_COLS, of_head(TOK_DEV), of_head(TOK_DEV), of_head(8), ATTN_ROWS, full,
         full, rel(D), rel(D)] + [rel(D // 2)] * 4,
        [BOTH_COLS, of_head(D), of_head(8), of_head(TOK_DEV)],
        [flat(2 * TOK_DEV, BF16), per_head(D, BF16), per_head(8, F32), per_head(TOK_DEV, BF16)],
        3 + 7, 15, [pltpu.VMEM((D, SCORES), F32)],
    )(where, scale, q, h2, p, pf, inv, attn, m_own, m_oth, *weights)


def near_backward(scale, q, k, v, h1, h2, p, pf, g, delta, dscore):
    return call(
        near_grad_kernel, 1,
        [HEAD_COLS, KV_COLS, KV_COLS, BOTH_COLS, KV_COLS, of_head(2 * TOK_DEV),
         of_head(2 * TOK_DEV), of_head(D), of_head(8), of_head(TOK_DEV)],
        [HEAD_COLS, BOTH_COLS, BOTH_COLS, pl.BlockSpec((8, 128), lambda h, *_: (h, 0))],
        [jax.ShapeDtypeStruct((TOK_DEV, WIDTH), BF16), flat(2 * TOK_DEV, F32),
         flat(2 * TOK_DEV, BF16), jax.ShapeDtypeStruct((8 * KV_HEADS, 128), F32)],
        9, 13,
    )(scale, q, k, v, h1, h2, p, pf, g, delta, dscore)


def weight_product(where, a_own, a_oth, m0, m1, m3, m2a, m2b):
    vmem = pl.BlockSpec(memory_space=pltpu.VMEM)
    return pl.pallas_call(
        weight_kernel,
        in_specs=[pl.BlockSpec(memory_space=pltpu.SMEM)] + [vmem] * 7,
        out_specs=vmem,
        out_shape=jax.ShapeDtypeStruct((4, 128, HALF), BF16),
        cost_estimate=pl.CostEstimate(
            flops=2 * 512 * HALF * 2048, transcendentals=0, bytes_accessed=7 << 20
        ),
        name="weight_product",
    )(where, a_own, a_oth, m0, m1, m3, m2a, m2b)


def all_steps(queries, keys, values, out_grad, out_weight, seq_len):
    q_rows = queries[0]
    k_rows = keys[0]
    v_rows = values[0]
    length = seq_len[0]
    core = lax.axis_index("dp_1")
    x_hi = lax.axis_index("dp_0")
    x_lo = lax.axis_index("seq_1")
    index = lax.axis_index(SEQ)
    start = index * TOK_DEV
    where = jnp.stack([index, lax.axis_index("seq_0"), x_lo, 2 * x_hi + x_lo]).astype(jnp.int32)

    kv = jnp.concatenate([k_rows, v_rows], 0)
    h1 = shifted(kv, 1)
    h2 = shifted(h1, 1)

    slots = TOK_DEV * lax.axis_size(SEQ) * lax.axis_size(DP)
    count = jnp.clip(length, 0, TOK_DEV * lax.axis_size(SEQ)).astype(F32).reshape(1)
    count = count + swap(count, "dp_1")
    count = count + swap(count, "dp_0")
    act_scale = slots / count
    weight_scale = lax.rsqrt(count[0])

    half_of = lambda a, c: lax.dynamic_slice_in_dim(a, c * HALF, HALF, 1)
    valid = (start + jnp.arange(TOK_DEV, dtype=jnp.int32)) < length
    masked = jnp.where(valid[:, None], out_grad[0], jnp.zeros((), BF16))
    m_own = half_of(masked, core)
    m_oth = half_of(masked, 1 - core)
    m0 = jnp.concatenate([m_own, swap(m_oth, "dp_1")], 0)
    m1 = ring(m0, "seq_0", 1)
    m3 = ring(m0, "seq_0", -1)
    m2a = ring(m1[:TOK_DEV], "seq_0", 1)
    m2b = ring(m3[TOK_DEV:], "seq_0", -1)

    w_z = for_each(half_of(out_weight, core), "seq_2").reshape(HEAD_DIM, HALF)
    w_up = ring(w_z, "seq_0", 1)
    w_down = ring(w_z, "seq_0", -1)
    mid = HEAD_DIM // 2
    w_far = [ring(w_up[:mid], "seq_0", 1), ring(w_down[mid:], "seq_0", -1)]
    wa = jnp.stack([w_z, w_up, jnp.concatenate(w_far, 0), w_down])
    wbl = across_x(wa[:, :mid], 1)
    wbh = across_x(wa[:, mid:], -1)
    wc = swap(wa, "dp_1")
    wdl = swap(wbl, "dp_1")
    wdh = swap(wbh, "dp_1")

    p, pf, acc, tot = near_forward(where, q_rows, k_rows, v_rows, h1)
    p2, pf2, attn, inv = far_forward(where, q_rows, h2, acc, tot)
    a_own = jnp.stack([
        attn[0], ring(attn[1], "seq_0", 1), ring(attn[2], "seq_0", 2), ring(attn[3], "seq_0", -1)
    ])
    a_oth = swap(a_own, "dp_1")

    d2, g, delta, dscore = far_backward(
        where, act_scale, q_rows, h2, p2, pf2, inv, attn, m_own, m_oth,
        (wa, wc, wbl, wbh, wdl, wdh),
    )
    r1 = shifted(d2, -1)
    dq, d0, d1, dq_sq = near_backward(
        act_scale, q_rows, k_rows, v_rows, h1, h2, p, pf, g, delta, dscore
    )
    r2 = shifted((d1.astype(F32) + r1.astype(F32)).astype(BF16), -1)
    dkv = d0 + r2.astype(F32)
    square = jnp.sum(dkv * dkv) + jnp.sum(dq_sq.reshape(KV_HEADS, 8, 128)[:, 0, 0])
    dkv = dkv.astype(BF16)

    part = weight_product(
        where, a_own, a_oth, m0, m1, m3, m2a, m2b
    )
    part = (
        part[0].astype(F32)
        + ring_x(part[1], 1).astype(F32)
        + ring_x(part[2], 2).astype(F32)
        + ring_x(part[3], -1).astype(F32)
    ).astype(BF16)
    pieces = lax.all_to_all(part, "seq_2", 0, 0, tiled=True)
    piece = jnp.sum(pieces.reshape(8, 16, HALF).astype(F32), axis=0) * weight_scale
    square = square + jnp.sum(piece * piece)

    other = swap(piece, "dp_1")
    row = jnp.where(
        core == 0, jnp.concatenate([piece, other], 1), jnp.concatenate([other, piece], 1)
    )
    other = swap(row, "dp_0")
    weight_grad = jnp.where(
        x_hi == 0, jnp.concatenate([row, other], 0), jnp.concatenate([other, row], 0)
    )

    square = jnp.full((8, 128), square, F32)
    square = for_each(square, ("dp_0", "seq_1", "dp_1"))
    square = jnp.full((8, 128), jnp.sum(square[:, 0], axis=0)[0], F32)
    square = for_each(square, ("seq_0", "seq_2"))
    square = jnp.sum(square[:, 0], axis=0)[0]
    entries = slots * (HEADS + 2 * KV_HEADS) * HEAD_DIM + WIDTH * D_OUT
    grad_rms = jnp.sqrt(square / entries)
    return (dq[None], dkv[:TOK_DEV][None], dkv[TOK_DEV:][None], weight_grad, grad_rms)


def solution(mesh):
    split = Mesh(mesh.devices.reshape(4, 2, 8, 2, 2), ("seq_0", "seq_1", "seq_2", "dp_0", "dp_1"))
    placed = (
        P(DP, SEQ, None),
        P(DP, SEQ, None),
        P(DP, SEQ, None),
        P(DP, SEQ, None),
        P(SEQ, None),
        P(DP),
    )
    return jax.shard_map(
        all_steps,
        mesh=split,
        in_specs=placed,
        out_specs=(P(DP, SEQ, None), P(DP, SEQ, None), P(DP, SEQ, None), P(SEQ, None), P()),
        check_vma=False,
    )
```

```python
import math

import jax
import jax.numpy as jnp
from jax import lax
from jax.experimental import pallas as pl
from jax.experimental.pallas import tpu as pltpu
from jax.sharding import Mesh
from jax.sharding import PartitionSpec as P


HEADS = 8
KV_HEADS = 4
GROUP = HEADS // KV_HEADS
HEAD_DIM = 256
D_OUT = 1792
HALF = D_OUT // 2
TOK_DEV = 256
WIDTH = HEADS * HEAD_DIM
SEQ = ("seq_0", "seq_1", "seq_2")
DP = ("dp_0", "dp_1")
X_AXES = ("seq_1", "dp_0")
SCALE = 0.0625
CAP = 50.0
EXP_MUL = CAP * math.log2(math.e)
BF16 = jnp.bfloat16
F32 = jnp.float32


def shifted(value, steps):
    count = lax.axis_size(SEQ)
    initial, last = (max(0, -steps), min(count, count - steps))
    return lax.ppermute(value, SEQ, [(source, source + steps) for source in range(initial, last)])


def ring(value, axis, steps):
    count = lax.axis_size(axis)
    return lax.ppermute(value, axis, [(s, (s + steps) % count) for s in range(count)])


def ring_x(value, steps):
    at = lambda x: (x % 2) * 2 + x // 2
    return lax.ppermute(value, X_AXES, [(at(s), at((s + steps) % 4)) for s in range(4)])


def across_x(value, steps):
    pairs = []
    depth = lax.axis_size("seq_2")
    for low in range(2):
        for z in range(depth):
            for high in range(2):
                step = steps if z else (1 if low else -1)
                to = (2 * high + low + step) % 4
                pairs.append(
                    ((low * depth + z) * 2 + high, ((to % 2) * depth + z) * 2 + to // 2)
                )
    return lax.ppermute(value, ("seq_1", "seq_2", "dp_0"), pairs)


def swap(value, axis):
    return lax.ppermute(value, axis, [(0, 1), (1, 0)])


def for_each(value, axis):
    size = lax.axis_size(axis)
    return lax.all_to_all(
        jnp.broadcast_to(value[None], (size, *value.shape)), axis, 0, 0, tiled=True
    )


def dot(a, b, dims):
    return lax.dot_general(a, b, (dims, ((), ())), preferred_element_type=F32)


NT = ((1,), (1,))
NN = ((1,), (0,))
TN = ((0,), (0,))


def squashed(k, q):
    t = jnp.tanh(dot(k, q, NT) * (SCALE / CAP))
    return t, jnp.exp2(t * EXP_MUL)


def places():
    shape = (TOK_DEV, GROUP * TOK_DEV)
    key = lax.broadcasted_iota(jnp.int32, shape, 0)
    query = lax.broadcasted_iota(jnp.int32, shape, 1) & (TOK_DEV - 1)
    return key, query


def two_heads(q_ref):
    return jnp.concatenate([q_ref[:, h * HEAD_DIM : (h + 1) * HEAD_DIM] for h in range(GROUP)], 0)


def row_sum(e):
    return jnp.sum(e, axis=0, keepdims=True)


def near_kernel(at_ref, q_ref, k0_ref, v0_ref, h1_ref, p_ref, pf_ref, acc_ref, tot_ref):
    q = two_heads(q_ref)
    key, query = places()
    t, e = squashed(h1_ref[:TOK_DEV], q)
    e = e * jnp.where(at_ref[0] >= 1, 1.0, 0.0)
    p1 = e.astype(BF16)
    p_ref[0, :TOK_DEV] = p1
    pf_ref[0, :TOK_DEV] = (e * (1.0 - t * t)).astype(BF16)
    total = row_sum(e)
    t, e = squashed(k0_ref[...], q)
    e = jnp.where(key <= query, e, 0.0)
    p0 = e.astype(BF16)
    p_ref[0, TOK_DEV:] = p0
    pf_ref[0, TOK_DEV:] = (e * (1.0 - t * t)).astype(BF16)
    total = total + row_sum(e)
    acc_ref[0] = dot(h1_ref[TOK_DEV:], p1, TN) + dot(v0_ref[...], p0, TN)
    tot_ref[0] = jnp.broadcast_to(total, tot_ref.shape[1:])


def far_kernel(at_ref, q_ref, h2_ref, acc_ref, tot_ref, p_ref, pf_ref, attn_ref, inv_ref):
    key, query = places()
    t, e = squashed(h2_ref[:TOK_DEV], two_heads(q_ref))
    e = jnp.where(key > query + jnp.where(at_ref[0] >= 2, 0, 4 * TOK_DEV), e, 0.0)
    p = e.astype(BF16)
    p_ref[0] = p
    pf_ref[0] = (e * (1.0 - t * t)).astype(BF16)
    inverse = 1.0 / (tot_ref[0, :1] + row_sum(e))
    inv_ref[0] = jnp.broadcast_to(inverse, inv_ref.shape[1:])
    out = ((acc_ref[0] + dot(h2_ref[TOK_DEV:], p, TN)) * inverse).astype(BF16)
    for h in range(GROUP):
        attn_ref[0, h * HEAD_DIM : (h + 1) * HEAD_DIM, :] = out[:, h * TOK_DEV : (h + 1) * TOK_DEV]


def score_terms(v, g, delta, pf):
    return (pf.astype(F32) * (dot(v, g, NN) - delta)).astype(BF16)


def far_grad_kernel(
    at_ref, scale_ref, q_ref, h2_ref, p_ref, pf_ref, inv_ref, attn_ref, m_own_ref, m_oth_ref,
    wa_ref, wc_ref, wbl_ref, wbh_ref, wdl_ref, wdh_ref,
    d2_ref, g_ref, delta_ref, ds_ref, raw_ref,
):
    act_scale = scale_ref[0]
    own = pl.multiple_of(at_ref[2] * TOK_DEV, TOK_DEV)
    oth = pl.multiple_of((1 - at_ref[2]) * TOK_DEV, TOK_DEV)
    both = dot(
        jnp.concatenate([wa_ref[0], wbl_ref[0], wbh_ref[0]], 0), m_own_ref[...], NT
    ) + dot(jnp.concatenate([wc_ref[0], wdl_ref[0], wdh_ref[0]], 0), m_oth_ref[...], NT)
    raw_ref[:, pl.ds(own, TOK_DEV)] = both[:HEAD_DIM]
    raw_ref[:, pl.ds(oth, TOK_DEV)] = both[HEAD_DIM:]
    g = (raw_ref[...] * inv_ref[0, :1]).astype(BF16)
    g_ref[0] = g
    attn = jnp.concatenate(
        [attn_ref[0, h * HEAD_DIM : (h + 1) * HEAD_DIM, :] for h in range(GROUP)], 1
    )
    delta = row_sum(g.astype(F32) * attn.astype(F32))
    delta_ref[0] = jnp.broadcast_to(delta, delta_ref.shape[1:])
    dscore = score_terms(h2_ref[TOK_DEV:], g, delta, pf_ref[0])
    ds_ref[0] = dscore
    d2_ref[:TOK_DEV] = (dot(dscore, two_heads(q_ref), NN) * (SCALE * act_scale)).astype(BF16)
    d2_ref[TOK_DEV:] = (dot(p_ref[0], g, NT) * act_scale).astype(BF16)


def near_grad_kernel(
    scale_ref, q_ref, k0_ref, v0_ref, h1_ref, h2_ref, p_ref, pf_ref, g_ref, delta_ref, ds_ref,
    dq_ref, d0_ref, d1_ref, sq_ref,
):
    act_scale = scale_ref[0]
    q = two_heads(q_ref)
    g = g_ref[0]
    delta = delta_ref[0, :1]
    dq = dot(h2_ref[...], ds_ref[0], TN)
    for k, v, at, out in (
        (h1_ref[:TOK_DEV], h1_ref[TOK_DEV:], 0, d1_ref),
        (k0_ref[...], v0_ref[...], TOK_DEV, d0_ref),
    ):
        dscore = score_terms(v, g, delta, pf_ref[0, at : at + TOK_DEV])
        dq = dq + dot(k, dscore, TN)
        out[:TOK_DEV] = (dot(dscore, q, NN) * (SCALE * act_scale)).astype(out.dtype)
        out[TOK_DEV:] = (dot(p_ref[0, at : at + TOK_DEV], g, NT) * act_scale).astype(out.dtype)
    dq = dq * (SCALE * act_scale)
    sq_ref[...] = jnp.broadcast_to(jnp.sum(dq * dq), sq_ref.shape)
    for h in range(GROUP):
        dq_ref[:, h * HEAD_DIM : (h + 1) * HEAD_DIM] = dq[
            :, h * TOK_DEV : (h + 1) * TOK_DEV
        ].T.astype(BF16)


def weight_kernel(at_ref, a_own_ref, a_oth_ref, m0_ref, m1_ref, m3_ref, m2a_ref, m2b_ref, out_ref):
    acc = None
    for back, (own, oth) in enumerate(
        (
            (m0_ref[:TOK_DEV], m0_ref[TOK_DEV:]),
            (m1_ref[:TOK_DEV], m1_ref[TOK_DEV:]),
            (m2a_ref[...], m2b_ref[...]),
            (m3_ref[:TOK_DEV], m3_ref[TOK_DEV:]),
        )
    ):
        both = dot(a_own_ref[back], own, NN) + dot(a_oth_ref[back], oth, NN)
        acc = both if acc is None else acc + both
    acc = acc.reshape(2, 8, 2, 16, HALF)
    for low in range(2):
        for high in range(2):
            away = (2 * high + low + 4 - at_ref[3]) % 4
            out_ref[away] = acc[low, :, high].reshape(128, HALF).astype(BF16)


D = HEAD_DIM
SCORES = GROUP * TOK_DEV
HEAD_COLS = pl.BlockSpec((TOK_DEV, GROUP * D), lambda h, *_: (0, h))
KV_COLS = pl.BlockSpec((TOK_DEV, D), lambda h, *_: (0, h))
BOTH_COLS = pl.BlockSpec((2 * TOK_DEV, D), lambda h, *_: (0, h))
ATTN_ROWS = pl.BlockSpec((1, GROUP * D, TOK_DEV), lambda h, at, *_: ((h + 4 - at[1]) % 4, 0, 0))


def of_head(rows, columns=SCORES):
    return pl.BlockSpec((1, rows, columns), lambda h, *_: (h, 0, 0))


def per_head(rows, dtype):
    return jax.ShapeDtypeStruct((KV_HEADS, rows, SCORES), dtype)


def flat(rows, dtype):
    return jax.ShapeDtypeStruct((rows, KV_HEADS * D), dtype)


def call(kernel, scalars, in_specs, out_specs, out_shape, products, mib, scratch=()):
    return pl.pallas_call(
        kernel,
        grid_spec=pltpu.PrefetchScalarGridSpec(
            num_scalar_prefetch=scalars,
            grid=(KV_HEADS,),
            in_specs=in_specs,
            out_specs=out_specs,
            scratch_shapes=scratch,
        ),
        out_shape=out_shape,
        cost_estimate=pl.CostEstimate(
            flops=products * 2 * HEADS * TOK_DEV**3, transcendentals=0, bytes_accessed=mib << 20
        ),
    )


def near_forward(where, q, k, v, h1):
    return call(
        near_kernel, 1,
        [HEAD_COLS, KV_COLS, KV_COLS, BOTH_COLS],
        [of_head(2 * TOK_DEV), of_head(2 * TOK_DEV), of_head(D), of_head(8)],
        [per_head(2 * TOK_DEV, BF16), per_head(2 * TOK_DEV, BF16), per_head(D, F32),
         per_head(8, F32)],
        4, 9,
    )(where, q, k, v, h1)


def far_forward(where, q, h2, acc, tot):
    return call(
        far_kernel, 1,
        [HEAD_COLS, BOTH_COLS, of_head(D), of_head(8)],
        [of_head(TOK_DEV), of_head(TOK_DEV), ATTN_ROWS, of_head(8)],
        [per_head(TOK_DEV, BF16), per_head(TOK_DEV, BF16),
         jax.ShapeDtypeStruct((KV_HEADS, GROUP * D, TOK_DEV), BF16), per_head(8, F32)],
        2, 7,
    )(where, q, h2, acc, tot)


def far_backward(where, scale, q, h2, p, pf, inv, attn, m_own, m_oth, weights):
    full = pl.BlockSpec((TOK_DEV, HALF), lambda h, *_: (0, 0))
    rel = lambda rows: pl.BlockSpec((1, rows, HALF), lambda h, at, *_: ((at[1] + 4 - h) % 4, 0, 0))
    return call(
        far_grad_kernel, 2,
        [HEAD_COLS, BOTH_COLS, of_head(TOK_DEV), of_head(TOK_DEV), of_head(8), ATTN_ROWS, full,
         full, rel(D), rel(D)] + [rel(D // 2)] * 4,
        [BOTH_COLS, of_head(D), of_head(8), of_head(TOK_DEV)],
        [flat(2 * TOK_DEV, BF16), per_head(D, BF16), per_head(8, F32), per_head(TOK_DEV, BF16)],
        3 + 7, 15, [pltpu.VMEM((D, SCORES), F32)],
    )(where, scale, q, h2, p, pf, inv, attn, m_own, m_oth, *weights)


def near_backward(scale, q, k, v, h1, h2, p, pf, g, delta, dscore):
    return call(
        near_grad_kernel, 1,
        [HEAD_COLS, KV_COLS, KV_COLS, BOTH_COLS, KV_COLS, of_head(2 * TOK_DEV),
         of_head(2 * TOK_DEV), of_head(D), of_head(8), of_head(TOK_DEV)],
        [HEAD_COLS, BOTH_COLS, BOTH_COLS, pl.BlockSpec((8, 128), lambda h, *_: (h, 0))],
        [jax.ShapeDtypeStruct((TOK_DEV, WIDTH), BF16), flat(2 * TOK_DEV, F32),
         flat(2 * TOK_DEV, BF16), jax.ShapeDtypeStruct((8 * KV_HEADS, 128), F32)],
        9, 13,
    )(scale, q, k, v, h1, h2, p, pf, g, delta, dscore)


def weight_product(where, a_own, a_oth, m0, m1, m3, m2a, m2b):
    vmem = pl.BlockSpec(memory_space=pltpu.VMEM)
    return pl.pallas_call(
        weight_kernel,
        in_specs=[pl.BlockSpec(memory_space=pltpu.SMEM)] + [vmem] * 7,
        out_specs=vmem,
        out_shape=jax.ShapeDtypeStruct((4, 128, HALF), BF16),
        cost_estimate=pl.CostEstimate(
            flops=2 * 512 * HALF * 2048, transcendentals=0, bytes_accessed=7 << 20
        ),
        name="weight_product",
    )(where, a_own, a_oth, m0, m1, m3, m2a, m2b)


def all_steps(queries, keys, values, out_grad, out_weight, seq_len):
    q_rows = queries[0]
    k_rows = keys[0]
    v_rows = values[0]
    length = seq_len[0]
    core = lax.axis_index("dp_1")
    x_hi = lax.axis_index("dp_0")
    x_lo = lax.axis_index("seq_1")
    index = lax.axis_index(SEQ)
    start = index * TOK_DEV
    where = jnp.stack([index, lax.axis_index("seq_0"), x_lo, 2 * x_hi + x_lo]).astype(jnp.int32)

    kv = jnp.concatenate([k_rows, v_rows], 0)
    h1 = shifted(kv, 1)
    h2 = shifted(h1, 1)

    slots = TOK_DEV * lax.axis_size(SEQ) * lax.axis_size(DP)
    count = jnp.clip(length, 0, TOK_DEV * lax.axis_size(SEQ)).astype(F32).reshape(1)
    count = count + swap(count, "dp_1")
    count = count + swap(count, "dp_0")
    act_scale = slots / count
    weight_scale = lax.rsqrt(count[0])

    half_of = lambda a, c: lax.dynamic_slice_in_dim(a, c * HALF, HALF, 1)
    valid = (start + jnp.arange(TOK_DEV, dtype=jnp.int32)) < length
    masked = jnp.where(valid[:, None], out_grad[0], jnp.zeros((), BF16))
    m_own = half_of(masked, core)
    m_oth = half_of(masked, 1 - core)
    m0 = jnp.concatenate([m_own, swap(m_oth, "dp_1")], 0)
    m1 = ring(m0, "seq_0", 1)
    m3 = ring(m0, "seq_0", -1)
    m2a = ring(m1[:TOK_DEV], "seq_0", 1)
    m2b = ring(m3[TOK_DEV:], "seq_0", -1)

    w_z = for_each(half_of(out_weight, core), "seq_2").reshape(HEAD_DIM, HALF)
    w_up = ring(w_z, "seq_0", 1)
    w_down = ring(w_z, "seq_0", -1)
    mid = HEAD_DIM // 2
    w_far = [ring(w_up[:mid], "seq_0", 1), ring(w_down[mid:], "seq_0", -1)]
    wa = jnp.stack([w_z, w_up, jnp.concatenate(w_far, 0), w_down])
    wbl = across_x(wa[:, :mid], 1)
    wbh = across_x(wa[:, mid:], -1)
    wc = swap(wa, "dp_1")
    wdl = swap(wbl, "dp_1")
    wdh = swap(wbh, "dp_1")

    p, pf, acc, tot = near_forward(where, q_rows, k_rows, v_rows, h1)
    p2, pf2, attn, inv = far_forward(where, q_rows, h2, acc, tot)
    attn_parts = (
        attn[0], ring(attn[1], "seq_0", 1), ring(attn[2], "seq_0", 2), ring(attn[3], "seq_0", -1)
    )

    d2, g, delta, dscore = far_backward(
        where, act_scale, q_rows, h2, p2, pf2, inv, attn, m_own, m_oth,
        (wa, wc, wbl, wbh, wdl, wdh),
    )
    attn_parts, _ = lax.optimization_barrier((attn_parts, delta))
    a_own = jnp.stack(attn_parts)
    a_oth = swap(a_own, "dp_1")

    r1 = shifted(d2, -1)
    dq, d0, d1, dq_sq = near_backward(
        act_scale, q_rows, k_rows, v_rows, h1, h2, p, pf, g, delta, dscore
    )
    r2 = shifted((d1.astype(F32) + r1.astype(F32)).astype(BF16), -1)
    dkv = d0 + r2.astype(F32)
    square = jnp.sum(dkv * dkv) + jnp.sum(dq_sq.reshape(KV_HEADS, 8, 128)[:, 0, 0])
    dkv = dkv.astype(BF16)

    part = weight_product(
        where, a_own, a_oth, m0, m1, m3, m2a, m2b
    )
    part = (
        part[0].astype(F32)
        + ring_x(part[1], 1).astype(F32)
        + ring_x(part[2], 2).astype(F32)
        + ring_x(part[3], -1).astype(F32)
    ).astype(BF16)
    pieces = lax.all_to_all(part, "seq_2", 0, 0, tiled=True)
    piece = jnp.sum(pieces.reshape(8, 16, HALF).astype(F32), axis=0) * weight_scale
    square = square + jnp.sum(piece * piece)

    other = swap(piece, "dp_1")
    row = jnp.where(
        core == 0, jnp.concatenate([piece, other], 1), jnp.concatenate([other, piece], 1)
    )
    other = swap(row, "dp_0")
    weight_grad = jnp.where(
        x_hi == 0, jnp.concatenate([row, other], 0), jnp.concatenate([other, row], 0)
    )

    square = jnp.full((8, 128), square, F32)
    square = for_each(square, ("dp_0", "seq_1", "dp_1"))
    square = jnp.full((8, 128), jnp.sum(square[:, 0], axis=0)[0], F32)
    square = for_each(square, ("seq_0", "seq_2"))
    square = jnp.sum(square[:, 0], axis=0)[0]
    entries = slots * (HEADS + 2 * KV_HEADS) * HEAD_DIM + WIDTH * D_OUT
    grad_rms = jnp.sqrt(square / entries)
    return (dq[None], dkv[:TOK_DEV][None], dkv[TOK_DEV:][None], weight_grad, grad_rms)


def solution(mesh):
    split = Mesh(mesh.devices.reshape(4, 2, 8, 2, 2), ("seq_0", "seq_1", "seq_2", "dp_0", "dp_1"))
    placed = (
        P(DP, SEQ, None),
        P(DP, SEQ, None),
        P(DP, SEQ, None),
        P(DP, SEQ, None),
        P(SEQ, None),
        P(DP),
    )
    return jax.shard_map(
        all_steps,
        mesh=split,
        in_specs=placed,
        out_specs=(P(DP, SEQ, None), P(DP, SEQ, None), P(DP, SEQ, None), P(SEQ, None), P()),
        check_vma=False,
    )
```

```python
import math

import jax
import jax.numpy as jnp
from jax import lax
from jax.experimental import pallas as pl
from jax.experimental.pallas import tpu as pltpu
from jax.sharding import Mesh
from jax.sharding import PartitionSpec as P


HEADS = 8
KV_HEADS = 4
GROUP = HEADS // KV_HEADS
HEAD_DIM = 256
D_OUT = 1792
HALF = D_OUT // 2
TOK_DEV = 256
WIDTH = HEADS * HEAD_DIM
SEQ = ("seq_0", "seq_1", "seq_2")
DP = ("dp_0", "dp_1")
X_AXES = ("seq_1", "dp_0")
SCALE = 0.0625
CAP = 50.0
EXP_MUL = CAP * math.log2(math.e)
BF16 = jnp.bfloat16
F32 = jnp.float32


def shifted(value, steps):
    count = lax.axis_size(SEQ)
    initial, last = (max(0, -steps), min(count, count - steps))
    return lax.ppermute(value, SEQ, [(source, source + steps) for source in range(initial, last)])


def ring(value, axis, steps):
    count = lax.axis_size(axis)
    return lax.ppermute(value, axis, [(s, (s + steps) % count) for s in range(count)])


def ring_x(value, steps):
    at = lambda x: (x % 2) * 2 + x // 2
    return lax.ppermute(value, X_AXES, [(at(s), at((s + steps) % 4)) for s in range(4)])


def across_x(value, steps):
    pairs = []
    depth = lax.axis_size("seq_2")
    for low in range(2):
        for z in range(depth):
            for high in range(2):
                step = steps if z else (1 if low else -1)
                to = (2 * high + low + step) % 4
                pairs.append(
                    ((low * depth + z) * 2 + high, ((to % 2) * depth + z) * 2 + to // 2)
                )
    return lax.ppermute(value, ("seq_1", "seq_2", "dp_0"), pairs)


def swap(value, axis):
    return lax.ppermute(value, axis, [(0, 1), (1, 0)])


def for_each(value, axis):
    size = lax.axis_size(axis)
    return lax.all_to_all(
        jnp.broadcast_to(value[None], (size, *value.shape)), axis, 0, 0, tiled=True
    )


def dot(a, b, dims):
    return lax.dot_general(a, b, (dims, ((), ())), preferred_element_type=F32)


NT = ((1,), (1,))
NN = ((1,), (0,))
TN = ((0,), (0,))


def squashed(k, q):
    t = jnp.tanh(dot(k, q, NT) * (SCALE / CAP))
    return t, jnp.exp2(t * EXP_MUL)


def places():
    shape = (TOK_DEV, GROUP * TOK_DEV)
    key = lax.broadcasted_iota(jnp.int32, shape, 0)
    query = lax.broadcasted_iota(jnp.int32, shape, 1) & (TOK_DEV - 1)
    return key, query


def two_heads(q_ref):
    return jnp.concatenate([q_ref[:, h * HEAD_DIM : (h + 1) * HEAD_DIM] for h in range(GROUP)], 0)


def row_sum(e):
    return jnp.sum(e, axis=0, keepdims=True)


def near_kernel(at_ref, q_ref, k0_ref, v0_ref, h1_ref, p_ref, pf_ref, acc_ref, tot_ref):
    q = two_heads(q_ref)
    key, query = places()
    t, e = squashed(h1_ref[:TOK_DEV], q)
    e = e * jnp.where(at_ref[0] >= 1, 1.0, 0.0)
    p1 = e.astype(BF16)
    p_ref[0, :TOK_DEV] = p1
    pf_ref[0, :TOK_DEV] = (e * (1.0 - t * t)).astype(BF16)
    total = row_sum(e)
    t, e = squashed(k0_ref[...], q)
    e = jnp.where(key <= query, e, 0.0)
    p0 = e.astype(BF16)
    p_ref[0, TOK_DEV:] = p0
    pf_ref[0, TOK_DEV:] = (e * (1.0 - t * t)).astype(BF16)
    total = total + row_sum(e)
    acc_ref[0] = dot(h1_ref[TOK_DEV:], p1, TN) + dot(v0_ref[...], p0, TN)
    tot_ref[0] = jnp.broadcast_to(total, tot_ref.shape[1:])


def far_kernel(at_ref, q_ref, h2_ref, acc_ref, tot_ref, p_ref, pf_ref, attn_ref, inv_ref):
    key, query = places()
    t, e = squashed(h2_ref[:TOK_DEV], two_heads(q_ref))
    e = jnp.where(key > query + jnp.where(at_ref[0] >= 2, 0, 4 * TOK_DEV), e, 0.0)
    p = e.astype(BF16)
    p_ref[0] = p
    pf_ref[0] = (e * (1.0 - t * t)).astype(BF16)
    inverse = 1.0 / (tot_ref[0, :1] + row_sum(e))
    inv_ref[0] = jnp.broadcast_to(inverse, inv_ref.shape[1:])
    out = ((acc_ref[0] + dot(h2_ref[TOK_DEV:], p, TN)) * inverse).astype(BF16)
    for h in range(GROUP):
        attn_ref[0, h * HEAD_DIM : (h + 1) * HEAD_DIM, :] = out[:, h * TOK_DEV : (h + 1) * TOK_DEV]


def score_terms(v, g, delta, pf):
    return (pf.astype(F32) * (dot(v, g, NN) - delta)).astype(BF16)


def far_grad_kernel(
    at_ref, scale_ref, q_ref, h2_ref, p_ref, pf_ref, inv_ref, attn_ref, m_own_ref, m_oth_ref,
    wa_ref, wc_ref, wbl_ref, wbh_ref, wdl_ref, wdh_ref,
    d2_ref, g_ref, delta_ref, ds_ref, raw_ref,
):
    act_scale = scale_ref[0]
    own = pl.multiple_of(at_ref[2] * TOK_DEV, TOK_DEV)
    oth = pl.multiple_of((1 - at_ref[2]) * TOK_DEV, TOK_DEV)
    both = dot(
        jnp.concatenate([wa_ref[0], wbl_ref[0], wbh_ref[0]], 0), m_own_ref[...], NT
    ) + dot(jnp.concatenate([wc_ref[0], wdl_ref[0], wdh_ref[0]], 0), m_oth_ref[...], NT)
    raw_ref[:, pl.ds(own, TOK_DEV)] = both[:HEAD_DIM]
    raw_ref[:, pl.ds(oth, TOK_DEV)] = both[HEAD_DIM:]
    g = (raw_ref[...] * inv_ref[0, :1]).astype(BF16)
    g_ref[0] = g
    attn = jnp.concatenate(
        [attn_ref[0, h * HEAD_DIM : (h + 1) * HEAD_DIM, :] for h in range(GROUP)], 1
    )
    delta = row_sum(g.astype(F32) * attn.astype(F32))
    delta_ref[0] = jnp.broadcast_to(delta, delta_ref.shape[1:])
    dscore = score_terms(h2_ref[TOK_DEV:], g, delta, pf_ref[0])
    ds_ref[0] = dscore
    d2_ref[:TOK_DEV] = (dot(dscore, two_heads(q_ref), NN) * (SCALE * act_scale)).astype(BF16)
    d2_ref[TOK_DEV:] = (dot(p_ref[0], g, NT) * act_scale).astype(BF16)


def near_grad_kernel(
    scale_ref, q_ref, k0_ref, v0_ref, h1_ref, h2_ref, p_ref, pf_ref, g_ref, delta_ref, ds_ref,
    dq_ref, d0_ref, d1_ref, sq_ref,
):
    act_scale = scale_ref[0]
    q = two_heads(q_ref)
    g = g_ref[0]
    delta = delta_ref[0, :1]
    dq = dot(h2_ref[...], ds_ref[0], TN)
    for k, v, at, out in (
        (h1_ref[:TOK_DEV], h1_ref[TOK_DEV:], 0, d1_ref),
        (k0_ref[...], v0_ref[...], TOK_DEV, d0_ref),
    ):
        dscore = score_terms(v, g, delta, pf_ref[0, at : at + TOK_DEV])
        dq = dq + dot(k, dscore, TN)
        out[:TOK_DEV] = (dot(dscore, q, NN) * (SCALE * act_scale)).astype(out.dtype)
        out[TOK_DEV:] = (dot(p_ref[0, at : at + TOK_DEV], g, NT) * act_scale).astype(out.dtype)
    dq = dq * (SCALE * act_scale)
    sq_ref[...] = jnp.broadcast_to(jnp.sum(dq * dq), sq_ref.shape)
    for h in range(GROUP):
        dq_ref[:, h * HEAD_DIM : (h + 1) * HEAD_DIM] = dq[
            :, h * TOK_DEV : (h + 1) * TOK_DEV
        ].T.astype(BF16)


def weight_kernel(at_ref, a_own_ref, a_oth_ref, m0_ref, m1_ref, m2_ref, m3_ref, out_ref):
    acc = None
    for back, m_ref in enumerate((m0_ref, m1_ref, m2_ref, m3_ref)):
        both = dot(a_own_ref[back], m_ref[:TOK_DEV], NN) + dot(
            a_oth_ref[back], m_ref[TOK_DEV:], NN
        )
        acc = both if acc is None else acc + both
    acc = acc.reshape(2, 8, 2, 16, HALF)
    for low in range(2):
        for high in range(2):
            away = (2 * high + low + 4 - at_ref[3]) % 4
            out_ref[away] = acc[low, :, high].reshape(128, HALF).astype(BF16)


D = HEAD_DIM
SCORES = GROUP * TOK_DEV
HEAD_COLS = pl.BlockSpec((TOK_DEV, GROUP * D), lambda h, *_: (0, h))
KV_COLS = pl.BlockSpec((TOK_DEV, D), lambda h, *_: (0, h))
BOTH_COLS = pl.BlockSpec((2 * TOK_DEV, D), lambda h, *_: (0, h))
ATTN_ROWS = pl.BlockSpec((1, GROUP * D, TOK_DEV), lambda h, at, *_: ((h + 4 - at[1]) % 4, 0, 0))


def of_head(rows, columns=SCORES):
    return pl.BlockSpec((1, rows, columns), lambda h, *_: (h, 0, 0))


def per_head(rows, dtype):
    return jax.ShapeDtypeStruct((KV_HEADS, rows, SCORES), dtype)


def flat(rows, dtype):
    return jax.ShapeDtypeStruct((rows, KV_HEADS * D), dtype)


def call(kernel, scalars, in_specs, out_specs, out_shape, products, mib, scratch=()):
    return pl.pallas_call(
        kernel,
        grid_spec=pltpu.PrefetchScalarGridSpec(
            num_scalar_prefetch=scalars,
            grid=(KV_HEADS,),
            in_specs=in_specs,
            out_specs=out_specs,
            scratch_shapes=scratch,
        ),
        out_shape=out_shape,
        cost_estimate=pl.CostEstimate(
            flops=products * 2 * HEADS * TOK_DEV**3, transcendentals=0, bytes_accessed=mib << 20
        ),
    )


def near_forward(where, q, k, v, h1):
    return call(
        near_kernel, 1,
        [HEAD_COLS, KV_COLS, KV_COLS, BOTH_COLS],
        [of_head(2 * TOK_DEV), of_head(2 * TOK_DEV), of_head(D), of_head(8)],
        [per_head(2 * TOK_DEV, BF16), per_head(2 * TOK_DEV, BF16), per_head(D, F32),
         per_head(8, F32)],
        4, 9,
    )(where, q, k, v, h1)


def far_forward(where, q, h2, acc, tot):
    return call(
        far_kernel, 1,
        [HEAD_COLS, BOTH_COLS, of_head(D), of_head(8)],
        [of_head(TOK_DEV), of_head(TOK_DEV), ATTN_ROWS, of_head(8)],
        [per_head(TOK_DEV, BF16), per_head(TOK_DEV, BF16),
         jax.ShapeDtypeStruct((KV_HEADS, GROUP * D, TOK_DEV), BF16), per_head(8, F32)],
        2, 7,
    )(where, q, h2, acc, tot)


def far_backward(where, scale, q, h2, p, pf, inv, attn, m_own, m_oth, weights):
    full = pl.BlockSpec((TOK_DEV, HALF), lambda h, *_: (0, 0))
    rel = lambda rows: pl.BlockSpec((1, rows, HALF), lambda h, at, *_: ((at[1] + 4 - h) % 4, 0, 0))
    return call(
        far_grad_kernel, 2,
        [HEAD_COLS, BOTH_COLS, of_head(TOK_DEV), of_head(TOK_DEV), of_head(8), ATTN_ROWS, full,
         full, rel(D), rel(D)] + [rel(D // 2)] * 4,
        [BOTH_COLS, of_head(D), of_head(8), of_head(TOK_DEV)],
        [flat(2 * TOK_DEV, BF16), per_head(D, BF16), per_head(8, F32), per_head(TOK_DEV, BF16)],
        3 + 7, 15, [pltpu.VMEM((D, SCORES), F32)],
    )(where, scale, q, h2, p, pf, inv, attn, m_own, m_oth, *weights)


def near_backward(scale, q, k, v, h1, h2, p, pf, g, delta, dscore):
    return call(
        near_grad_kernel, 1,
        [HEAD_COLS, KV_COLS, KV_COLS, BOTH_COLS, KV_COLS, of_head(2 * TOK_DEV),
         of_head(2 * TOK_DEV), of_head(D), of_head(8), of_head(TOK_DEV)],
        [HEAD_COLS, BOTH_COLS, BOTH_COLS, pl.BlockSpec((8, 128), lambda h, *_: (h, 0))],
        [jax.ShapeDtypeStruct((TOK_DEV, WIDTH), BF16), flat(2 * TOK_DEV, F32),
         flat(2 * TOK_DEV, BF16), jax.ShapeDtypeStruct((8 * KV_HEADS, 128), F32)],
        9, 13,
    )(scale, q, k, v, h1, h2, p, pf, g, delta, dscore)


def weight_product(where, a_own, a_oth, m0, m1, m2, m3):
    vmem = pl.BlockSpec(memory_space=pltpu.VMEM)
    return pl.pallas_call(
        weight_kernel,
        in_specs=[pl.BlockSpec(memory_space=pltpu.SMEM)] + [vmem] * 6,
        out_specs=vmem,
        out_shape=jax.ShapeDtypeStruct((4, 128, HALF), BF16),
        cost_estimate=pl.CostEstimate(
            flops=2 * 512 * HALF * 2048, transcendentals=0, bytes_accessed=7 << 20
        ),
        name="weight_product",
    )(where, a_own, a_oth, m0, m1, m2, m3)


def all_steps(queries, keys, values, out_grad, out_weight, seq_len):
    q_rows = queries[0]
    k_rows = keys[0]
    v_rows = values[0]
    length = seq_len[0]
    core = lax.axis_index("dp_1")
    x_hi = lax.axis_index("dp_0")
    x_lo = lax.axis_index("seq_1")
    index = lax.axis_index(SEQ)
    start = index * TOK_DEV
    where = jnp.stack([index, lax.axis_index("seq_0"), x_lo, 2 * x_hi + x_lo]).astype(jnp.int32)

    kv = jnp.concatenate([k_rows, v_rows], 0)
    h1 = shifted(kv, 1)
    h2 = shifted(h1, 1)

    slots = TOK_DEV * lax.axis_size(SEQ) * lax.axis_size(DP)
    count = jnp.clip(length, 0, TOK_DEV * lax.axis_size(SEQ)).astype(F32).reshape(1)
    count = count + swap(count, "dp_1")
    count = count + swap(count, "dp_0")
    act_scale = slots / count
    weight_scale = lax.rsqrt(count[0])

    half_of = lambda a, c: lax.dynamic_slice_in_dim(a, c * HALF, HALF, 1)
    valid = (start + jnp.arange(TOK_DEV, dtype=jnp.int32)) < length
    masked = jnp.where(valid[:, None], out_grad[0], jnp.zeros((), BF16))
    m_own = half_of(masked, core)
    m_oth = half_of(masked, 1 - core)
    m0 = jnp.concatenate([m_own, swap(m_oth, "dp_1")], 0)
    m1 = ring(m0, "seq_0", 1)
    m3 = ring(m0, "seq_0", -1)
    m2 = ring(m3, "seq_0", -1)

    w_z = for_each(half_of(out_weight, core), "seq_2").reshape(HEAD_DIM, HALF)
    w_up = ring(w_z, "seq_0", 1)
    w_down = ring(w_z, "seq_0", -1)
    mid = HEAD_DIM // 2
    w_far = [ring(w_up[:mid], "seq_0", 1), ring(w_down[mid:], "seq_0", -1)]
    wa = jnp.stack([w_z, w_up, jnp.concatenate(w_far, 0), w_down])
    wbl = across_x(wa[:, :mid], 1)
    wbh = across_x(wa[:, mid:], -1)
    wc = swap(wa, "dp_1")
    wdl = swap(wbl, "dp_1")
    wdh = swap(wbh, "dp_1")

    p, pf, acc, tot = near_forward(where, q_rows, k_rows, v_rows, h1)
    p2, pf2, attn, inv = far_forward(where, q_rows, h2, acc, tot)
    attn_parts = (
        attn[0], ring(attn[1], "seq_0", 1), ring(attn[2], "seq_0", 2), ring(attn[3], "seq_0", -1)
    )

    d2, g, delta, dscore = far_backward(
        where, act_scale, q_rows, h2, p2, pf2, inv, attn, m_own, m_oth,
        (wa, wc, wbl, wbh, wdl, wdh),
    )
    attn_parts, _ = lax.optimization_barrier((attn_parts, delta))
    a_own = jnp.stack(attn_parts)
    a_oth = swap(a_own, "dp_1")

    r1 = shifted(d2, -1)
    dq, d0, d1, dq_sq = near_backward(
        act_scale, q_rows, k_rows, v_rows, h1, h2, p, pf, g, delta, dscore
    )
    r2 = shifted((d1.astype(F32) + r1.astype(F32)).astype(BF16), -1)
    dkv = d0 + r2.astype(F32)
    square = jnp.sum(dkv * dkv)
    square = square + jnp.sum(dq_sq.reshape(KV_HEADS, 8, 128)[:, 0, 0])
    dkv = dkv.astype(BF16)

    part = weight_product(
        where, a_own, a_oth, m0, m1, m2, m3
    )
    part = (
        part[0].astype(F32)
        + ring_x(part[1], 1).astype(F32)
        + ring_x(part[2], 2).astype(F32)
        + ring_x(part[3], -1).astype(F32)
    ).astype(BF16)
    pieces = lax.all_to_all(part, "seq_2", 0, 0, tiled=True)
    piece = jnp.sum(pieces.reshape(8, 16, HALF).astype(F32), axis=0) * weight_scale
    square = square + jnp.sum(piece * piece)

    other = swap(piece, "dp_1")
    row = jnp.where(
        core == 0, jnp.concatenate([piece, other], 1), jnp.concatenate([other, piece], 1)
    )
    other = swap(row, "dp_0")
    weight_grad = jnp.where(
        x_hi == 0, jnp.concatenate([row, other], 0), jnp.concatenate([other, row], 0)
    )

    square = jnp.full((8, 128), square, F32)
    square = for_each(square, ("dp_0", "seq_1", "dp_1"))
    square = jnp.full((8, 128), jnp.sum(square[:, 0], axis=0)[0], F32)
    square = for_each(square, ("seq_0", "seq_2"))
    square = jnp.sum(square[:, 0], axis=0)[0]
    entries = slots * (HEADS + 2 * KV_HEADS) * HEAD_DIM + WIDTH * D_OUT
    grad_rms = jnp.sqrt(square / entries)
    return (dq[None], dkv[:TOK_DEV][None], dkv[TOK_DEV:][None], weight_grad, grad_rms)


def solution(mesh):
    split = Mesh(mesh.devices.reshape(4, 2, 8, 2, 2), ("seq_0", "seq_1", "seq_2", "dp_0", "dp_1"))
    placed = (
        P(DP, SEQ, None),
        P(DP, SEQ, None),
        P(DP, SEQ, None),
        P(DP, SEQ, None),
        P(SEQ, None),
        P(DP),
    )
    return jax.shard_map(
        all_steps,
        mesh=split,
        in_specs=placed,
        out_specs=(P(DP, SEQ, None), P(DP, SEQ, None), P(DP, SEQ, None), P(SEQ, None), P()),
        check_vma=False,
    )
```

```python
import math

import jax
import jax.numpy as jnp
from jax import lax
from jax.experimental import pallas as pl
from jax.experimental.pallas import tpu as pltpu
from jax.sharding import Mesh
from jax.sharding import PartitionSpec as P


HEADS = 8
KV_HEADS = 4
GROUP = HEADS // KV_HEADS
HEAD_DIM = 256
D_OUT = 1792
HALF = D_OUT // 2
TOK_DEV = 256
WIDTH = HEADS * HEAD_DIM
SEQ = ("seq_0", "seq_1", "seq_2")
DP = ("dp_0", "dp_1")
X_AXES = ("seq_1", "dp_0")
SCALE = 0.0625
CAP = 50.0
EXP_MUL = CAP * math.log2(math.e)
BF16 = jnp.bfloat16
F32 = jnp.float32


def shifted(value, steps):
    count = lax.axis_size(SEQ)
    initial, last = (max(0, -steps), min(count, count - steps))
    return lax.ppermute(value, SEQ, [(source, source + steps) for source in range(initial, last)])


def ring(value, axis, steps):
    count = lax.axis_size(axis)
    return lax.ppermute(value, axis, [(s, (s + steps) % count) for s in range(count)])


def ring_x(value, steps):
    at = lambda x: (x % 2) * 2 + x // 2
    return lax.ppermute(value, X_AXES, [(at(s), at((s + steps) % 4)) for s in range(4)])


def across_x(value, steps):
    pairs = []
    depth = lax.axis_size("seq_2")
    for low in range(2):
        for z in range(depth):
            for high in range(2):
                step = steps if z else (1 if low else -1)
                to = (2 * high + low + step) % 4
                pairs.append(
                    ((low * depth + z) * 2 + high, ((to % 2) * depth + z) * 2 + to // 2)
                )
    return lax.ppermute(value, ("seq_1", "seq_2", "dp_0"), pairs)


def swap(value, axis):
    return lax.ppermute(value, axis, [(0, 1), (1, 0)])


def for_each(value, axis):
    size = lax.axis_size(axis)
    return lax.all_to_all(
        jnp.broadcast_to(value[None], (size, *value.shape)), axis, 0, 0, tiled=True
    )


def dot(a, b, dims):
    return lax.dot_general(a, b, (dims, ((), ())), preferred_element_type=F32)


NT = ((1,), (1,))
NN = ((1,), (0,))
TN = ((0,), (0,))


def squashed(k, q):
    t = jnp.tanh(dot(k, q, NT) * (SCALE / CAP))
    return t, jnp.exp2(t * EXP_MUL)


def places():
    shape = (TOK_DEV, GROUP * TOK_DEV)
    key = lax.broadcasted_iota(jnp.int32, shape, 0)
    query = lax.broadcasted_iota(jnp.int32, shape, 1) & (TOK_DEV - 1)
    return key, query


def two_heads(q_ref):
    return jnp.concatenate([q_ref[:, h * HEAD_DIM : (h + 1) * HEAD_DIM] for h in range(GROUP)], 0)


def row_sum(e):
    return jnp.sum(e, axis=0, keepdims=True)


def near_kernel(at_ref, q_ref, k0_ref, v0_ref, h1_ref, p_ref, pf_ref, acc_ref, tot_ref):
    q = two_heads(q_ref)
    key, query = places()
    t, e = squashed(h1_ref[:TOK_DEV], q)
    e = e * jnp.where(at_ref[0] >= 1, 1.0, 0.0)
    p1 = e.astype(BF16)
    p_ref[0, :TOK_DEV] = p1
    pf_ref[0, :TOK_DEV] = (e * (1.0 - t * t)).astype(BF16)
    total = row_sum(e)
    t, e = squashed(k0_ref[...], q)
    e = jnp.where(key <= query, e, 0.0)
    p0 = e.astype(BF16)
    p_ref[0, TOK_DEV:] = p0
    pf_ref[0, TOK_DEV:] = (e * (1.0 - t * t)).astype(BF16)
    total = total + row_sum(e)
    acc_ref[0] = dot(h1_ref[TOK_DEV:], p1, TN) + dot(v0_ref[...], p0, TN)
    tot_ref[0] = jnp.broadcast_to(total, tot_ref.shape[1:])


def far_kernel(
    at_ref, q_ref, h2_ref, acc_ref, tot_ref,
    p_ref, pf_ref, attn_ref, inv_ref, out0_ref, out1_ref, out2_ref, out3_ref,
):
    key, query = places()
    t, e = squashed(h2_ref[:TOK_DEV], two_heads(q_ref))
    e = jnp.where(key > query + jnp.where(at_ref[0] >= 2, 0, 4 * TOK_DEV), e, 0.0)
    p = e.astype(BF16)
    p_ref[0] = p
    pf_ref[0] = (e * (1.0 - t * t)).astype(BF16)
    inverse = 1.0 / (tot_ref[0, :1] + row_sum(e))
    inv_ref[0] = jnp.broadcast_to(inverse, inv_ref.shape[1:])
    out = ((acc_ref[0] + dot(h2_ref[TOK_DEV:], p, TN)) * inverse).astype(BF16)
    out = jnp.concatenate([out[:, h * TOK_DEV : (h + 1) * TOK_DEV] for h in range(GROUP)], 0)
    attn_ref[0] = out
    place = (pl.program_id(0) + 4 - at_ref[1]) % 4
    for away, out_ref in enumerate((out0_ref, out1_ref, out2_ref, out3_ref)):

        @pl.when(place == away)
        def _():
            out_ref[...] = out


def score_terms(v, g, delta, pf):
    return (pf.astype(F32) * (dot(v, g, NN) - delta)).astype(BF16)


def far_grad_kernel(
    at_ref, scale_ref, q_ref, h2_ref, p_ref, pf_ref, inv_ref, attn_ref, m_own_ref, m_oth_ref,
    wa_ref, wc_ref, wbl_ref, wbh_ref, wdl_ref, wdh_ref,
    d2_ref, g_ref, delta_ref, ds_ref, raw_ref,
):
    act_scale = scale_ref[0]
    own = pl.multiple_of(at_ref[2] * TOK_DEV, TOK_DEV)
    oth = pl.multiple_of((1 - at_ref[2]) * TOK_DEV, TOK_DEV)
    both = dot(
        jnp.concatenate([wa_ref[0], wbl_ref[0], wbh_ref[0]], 0), m_own_ref[...], NT
    ) + dot(jnp.concatenate([wc_ref[0], wdl_ref[0], wdh_ref[0]], 0), m_oth_ref[...], NT)
    raw_ref[:, pl.ds(own, TOK_DEV)] = both[:HEAD_DIM]
    raw_ref[:, pl.ds(oth, TOK_DEV)] = both[HEAD_DIM:]
    g = (raw_ref[...] * inv_ref[0, :1]).astype(BF16)
    g_ref[0] = g
    attn = jnp.concatenate(
        [attn_ref[0, h * HEAD_DIM : (h + 1) * HEAD_DIM, :] for h in range(GROUP)], 1
    )
    delta = row_sum(g.astype(F32) * attn.astype(F32))
    delta_ref[0] = jnp.broadcast_to(delta, delta_ref.shape[1:])
    dscore = score_terms(h2_ref[TOK_DEV:], g, delta, pf_ref[0])
    ds_ref[0] = dscore
    d2_ref[:TOK_DEV] = (dot(dscore, two_heads(q_ref), NN) * (SCALE * act_scale)).astype(BF16)
    d2_ref[TOK_DEV:] = (dot(p_ref[0], g, NT) * act_scale).astype(BF16)


def near_grad_kernel(
    scale_ref, q_ref, k0_ref, v0_ref, h1_ref, h2_ref, p_ref, pf_ref, g_ref, delta_ref, ds_ref,
    dq_ref, d0_ref, d1_ref, sq_ref,
):
    act_scale = scale_ref[0]
    q = two_heads(q_ref)
    g = g_ref[0]
    delta = delta_ref[0, :1]
    dq = dot(h2_ref[...], ds_ref[0], TN)
    for k, v, at, out in (
        (h1_ref[:TOK_DEV], h1_ref[TOK_DEV:], 0, d1_ref),
        (k0_ref[...], v0_ref[...], TOK_DEV, d0_ref),
    ):
        dscore = score_terms(v, g, delta, pf_ref[0, at : at + TOK_DEV])
        dq = dq + dot(k, dscore, TN)
        out[:TOK_DEV] = (dot(dscore, q, NN) * (SCALE * act_scale)).astype(out.dtype)
        out[TOK_DEV:] = (dot(p_ref[0, at : at + TOK_DEV], g, NT) * act_scale).astype(out.dtype)
    dq = dq * (SCALE * act_scale)
    sq_ref[...] = jnp.broadcast_to(jnp.sum(dq * dq), sq_ref.shape)
    for h in range(GROUP):
        dq_ref[:, h * HEAD_DIM : (h + 1) * HEAD_DIM] = dq[
            :, h * TOK_DEV : (h + 1) * TOK_DEV
        ].T.astype(BF16)


def weight_kernel(at_ref, a_own_ref, a_oth_ref, m0_ref, m1_ref, m2_ref, m3_ref, out_ref):
    acc = None
    for back, m_ref in enumerate((m0_ref, m1_ref, m2_ref, m3_ref)):
        both = dot(a_own_ref[back], m_ref[:TOK_DEV], NN) + dot(
            a_oth_ref[back], m_ref[TOK_DEV:], NN
        )
        acc = both if acc is None else acc + both
    acc = acc.reshape(2, 8, 2, 16, HALF)
    for low in range(2):
        for high in range(2):
            away = (2 * high + low + 4 - at_ref[3]) % 4
            out_ref[away] = acc[low, :, high].reshape(128, HALF).astype(BF16)


D = HEAD_DIM
SCORES = GROUP * TOK_DEV
HEAD_COLS = pl.BlockSpec((TOK_DEV, GROUP * D), lambda h, *_: (0, h))
KV_COLS = pl.BlockSpec((TOK_DEV, D), lambda h, *_: (0, h))
BOTH_COLS = pl.BlockSpec((2 * TOK_DEV, D), lambda h, *_: (0, h))
ATTN_ROWS = pl.BlockSpec((1, GROUP * D, TOK_DEV), lambda h, *_: (h, 0, 0))


def of_head(rows, columns=SCORES):
    return pl.BlockSpec((1, rows, columns), lambda h, *_: (h, 0, 0))


def per_head(rows, dtype):
    return jax.ShapeDtypeStruct((KV_HEADS, rows, SCORES), dtype)


def flat(rows, dtype):
    return jax.ShapeDtypeStruct((rows, KV_HEADS * D), dtype)


def call(kernel, scalars, in_specs, out_specs, out_shape, products, mib, scratch=()):
    return pl.pallas_call(
        kernel,
        grid_spec=pltpu.PrefetchScalarGridSpec(
            num_scalar_prefetch=scalars,
            grid=(KV_HEADS,),
            in_specs=in_specs,
            out_specs=out_specs,
            scratch_shapes=scratch,
        ),
        out_shape=out_shape,
        cost_estimate=pl.CostEstimate(
            flops=products * 2 * HEADS * TOK_DEV**3, transcendentals=0, bytes_accessed=mib << 20
        ),
    )


def near_forward(where, q, k, v, h1):
    return call(
        near_kernel, 1,
        [HEAD_COLS, KV_COLS, KV_COLS, BOTH_COLS],
        [of_head(2 * TOK_DEV), of_head(2 * TOK_DEV), of_head(D), of_head(8)],
        [per_head(2 * TOK_DEV, BF16), per_head(2 * TOK_DEV, BF16), per_head(D, F32),
         per_head(8, F32)],
        4, 9,
    )(where, q, k, v, h1)


def far_forward(where, q, h2, acc, tot):
    return call(
        far_kernel, 1,
        [HEAD_COLS, BOTH_COLS, of_head(D), of_head(8)],
        [of_head(TOK_DEV), of_head(TOK_DEV), ATTN_ROWS, of_head(8)]
        + [pl.BlockSpec((GROUP * D, TOK_DEV), lambda h, *_: (0, 0))] * 4,
        [per_head(TOK_DEV, BF16), per_head(TOK_DEV, BF16),
         jax.ShapeDtypeStruct((KV_HEADS, GROUP * D, TOK_DEV), BF16), per_head(8, F32)]
        + [jax.ShapeDtypeStruct((GROUP * D, TOK_DEV), BF16)] * 4,
        2, 7,
    )(where, q, h2, acc, tot)


def far_backward(where, scale, q, h2, p, pf, inv, attn, m_own, m_oth, weights):
    full = pl.BlockSpec((TOK_DEV, HALF), lambda h, *_: (0, 0))
    rel = lambda rows: pl.BlockSpec((1, rows, HALF), lambda h, at, *_: ((at[1] + 4 - h) % 4, 0, 0))
    return call(
        far_grad_kernel, 2,
        [HEAD_COLS, BOTH_COLS, of_head(TOK_DEV), of_head(TOK_DEV), of_head(8), ATTN_ROWS, full,
         full, rel(D), rel(D)] + [rel(D // 2)] * 4,
        [BOTH_COLS, of_head(D), of_head(8), of_head(TOK_DEV)],
        [flat(2 * TOK_DEV, BF16), per_head(D, BF16), per_head(8, F32), per_head(TOK_DEV, BF16)],
        3 + 7, 15, [pltpu.VMEM((D, SCORES), F32)],
    )(where, scale, q, h2, p, pf, inv, attn, m_own, m_oth, *weights)


def near_backward(scale, q, k, v, h1, h2, p, pf, g, delta, dscore):
    return call(
        near_grad_kernel, 1,
        [HEAD_COLS, KV_COLS, KV_COLS, BOTH_COLS, KV_COLS, of_head(2 * TOK_DEV),
         of_head(2 * TOK_DEV), of_head(D), of_head(8), of_head(TOK_DEV)],
        [HEAD_COLS, BOTH_COLS, BOTH_COLS, pl.BlockSpec((8, 128), lambda h, *_: (h, 0))],
        [jax.ShapeDtypeStruct((TOK_DEV, WIDTH), BF16), flat(2 * TOK_DEV, F32),
         flat(2 * TOK_DEV, BF16), jax.ShapeDtypeStruct((8 * KV_HEADS, 128), F32)],
        9, 13,
    )(scale, q, k, v, h1, h2, p, pf, g, delta, dscore)


def weight_product(where, a_own, a_oth, m0, m1, m2, m3):
    vmem = pl.BlockSpec(memory_space=pltpu.VMEM)
    return pl.pallas_call(
        weight_kernel,
        in_specs=[pl.BlockSpec(memory_space=pltpu.SMEM)] + [vmem] * 6,
        out_specs=vmem,
        out_shape=jax.ShapeDtypeStruct((4, 128, HALF), BF16),
        cost_estimate=pl.CostEstimate(
            flops=2 * 512 * HALF * 2048, transcendentals=0, bytes_accessed=7 << 20
        ),
        name="weight_product",
    )(where, a_own, a_oth, m0, m1, m2, m3)


def all_steps(queries, keys, values, out_grad, out_weight, seq_len):
    q_rows = queries[0]
    k_rows = keys[0]
    v_rows = values[0]
    length = seq_len[0]
    core = lax.axis_index("dp_1")
    x_hi = lax.axis_index("dp_0")
    x_lo = lax.axis_index("seq_1")
    index = lax.axis_index(SEQ)
    start = index * TOK_DEV
    where = jnp.stack([index, lax.axis_index("seq_0"), x_lo, 2 * x_hi + x_lo]).astype(jnp.int32)

    kv = jnp.concatenate([k_rows, v_rows], 0)
    h1 = shifted(kv, 1)
    h2 = shifted(h1, 1)

    slots = TOK_DEV * lax.axis_size(SEQ) * lax.axis_size(DP)
    count = jnp.clip(length, 0, TOK_DEV * lax.axis_size(SEQ)).astype(F32).reshape(1)
    count = count + swap(count, "dp_1")
    count = count + swap(count, "dp_0")
    act_scale = slots / count
    weight_scale = lax.rsqrt(count[0])

    half_of = lambda a, c: lax.dynamic_slice_in_dim(a, c * HALF, HALF, 1)
    valid = (start + jnp.arange(TOK_DEV, dtype=jnp.int32)) < length
    masked = jnp.where(valid[:, None], out_grad[0], jnp.zeros((), BF16))
    m_own = half_of(masked, core)
    m_oth = half_of(masked, 1 - core)
    m0 = jnp.concatenate([m_own, swap(m_oth, "dp_1")], 0)
    m1 = ring(m0, "seq_0", 1)
    m3 = ring(m0, "seq_0", -1)
    m2 = ring(m3, "seq_0", -1)

    w_z = for_each(half_of(out_weight, core), "seq_2").reshape(HEAD_DIM, HALF)
    w_up = ring(w_z, "seq_0", 1)
    w_down = ring(w_z, "seq_0", -1)
    mid = HEAD_DIM // 2
    w_far = [ring(w_up[:mid], "seq_0", 1), ring(w_down[mid:], "seq_0", -1)]
    wa = jnp.stack([w_z, w_up, jnp.concatenate(w_far, 0), w_down])
    wbl = across_x(wa[:, :mid], 1)
    wbh = across_x(wa[:, mid:], -1)
    wc = swap(wa, "dp_1")
    wdl = swap(wbl, "dp_1")
    wdh = swap(wbh, "dp_1")

    p, pf, acc, tot = near_forward(where, q_rows, k_rows, v_rows, h1)
    p2, pf2, attn, inv, *away = far_forward(where, q_rows, h2, acc, tot)
    attn_parts = (
        away[0], ring(away[1], "seq_0", 1), ring(away[2], "seq_0", 2), ring(away[3], "seq_0", -1)
    )

    d2, g, delta, dscore = far_backward(
        where, act_scale, q_rows, h2, p2, pf2, inv, attn, m_own, m_oth,
        (wa, wc, wbl, wbh, wdl, wdh),
    )
    attn_parts, _ = lax.optimization_barrier((attn_parts, delta))
    a_own = jnp.stack(attn_parts)
    a_oth = swap(a_own, "dp_1")

    r1 = shifted(d2, -1)
    dq, d0, d1, dq_sq = near_backward(
        act_scale, q_rows, k_rows, v_rows, h1, h2, p, pf, g, delta, dscore
    )
    part = weight_product(
        where, a_own, a_oth, m0, m1, m2, m3
    )
    r1, _ = lax.optimization_barrier((r1, part))
    r2 = shifted((d1.astype(F32) + r1.astype(F32)).astype(BF16), -1)
    dkv = d0 + r2.astype(F32)
    square = jnp.sum(dkv * dkv)
    square = square + jnp.sum(dq_sq.reshape(KV_HEADS, 8, 128)[:, 0, 0])
    dkv = dkv.astype(BF16)

    part = (
        part[0].astype(F32)
        + ring_x(part[1], 1).astype(F32)
        + ring_x(part[2], 2).astype(F32)
        + ring_x(part[3], -1).astype(F32)
    ).astype(BF16)
    pieces = lax.all_to_all(part, "seq_2", 0, 0, tiled=True)
    piece = jnp.sum(pieces.reshape(8, 16, HALF).astype(F32), axis=0) * weight_scale
    square = square + jnp.sum(piece * piece)

    other = swap(piece, "dp_1")
    row = jnp.where(
        core == 0, jnp.concatenate([piece, other], 1), jnp.concatenate([other, piece], 1)
    )
    other = swap(row, "dp_0")
    weight_grad = jnp.where(
        x_hi == 0, jnp.concatenate([row, other], 0), jnp.concatenate([other, row], 0)
    )

    square = jnp.full((8, 128), square, F32)
    square = for_each(square, ("dp_0", "seq_1", "dp_1"))
    square = jnp.full((8, 128), jnp.sum(square[:, 0], axis=0)[0], F32)
    square = for_each(square, ("seq_0", "seq_2"))
    square = jnp.sum(square[:, 0], axis=0)[0]
    entries = slots * (HEADS + 2 * KV_HEADS) * HEAD_DIM + WIDTH * D_OUT
    grad_rms = jnp.sqrt(square / entries)
    return (dq[None], dkv[:TOK_DEV][None], dkv[TOK_DEV:][None], weight_grad, grad_rms)


def solution(mesh):
    split = Mesh(mesh.devices.reshape(4, 2, 8, 2, 2), ("seq_0", "seq_1", "seq_2", "dp_0", "dp_1"))
    placed = (
        P(DP, SEQ, None),
        P(DP, SEQ, None),
        P(DP, SEQ, None),
        P(DP, SEQ, None),
        P(SEQ, None),
        P(DP),
    )
    return jax.shard_map(
        all_steps,
        mesh=split,
        in_specs=placed,
        out_specs=(P(DP, SEQ, None), P(DP, SEQ, None), P(DP, SEQ, None), P(SEQ, None), P()),
        check_vma=False,
    )
```

```python
import math

import jax
import jax.numpy as jnp
from jax import lax
from jax.experimental import pallas as pl
from jax.experimental.pallas import tpu as pltpu
from jax.sharding import Mesh
from jax.sharding import PartitionSpec as P


HEADS = 8
KV_HEADS = 4
GROUP = HEADS // KV_HEADS
HEAD_DIM = 256
D_OUT = 1792
HALF = D_OUT // 2
TOK_DEV = 256
WIDTH = HEADS * HEAD_DIM
SEQ = ("seq_0", "seq_1", "seq_2")
DP = ("dp_0", "dp_1")
X_AXES = ("seq_1", "dp_0")
SCALE = 0.0625
CAP = 50.0
EXP_MUL = CAP * math.log2(math.e)
BF16 = jnp.bfloat16
F32 = jnp.float32


def shifted(value, steps):
    count = lax.axis_size(SEQ)
    initial, last = (max(0, -steps), min(count, count - steps))
    return lax.ppermute(value, SEQ, [(source, source + steps) for source in range(initial, last)])


def ring(value, axis, steps):
    count = lax.axis_size(axis)
    return lax.ppermute(value, axis, [(s, (s + steps) % count) for s in range(count)])


def ring_x(value, steps):
    at = lambda x: (x % 2) * 2 + x // 2
    return lax.ppermute(value, X_AXES, [(at(s), at((s + steps) % 4)) for s in range(4)])


def next_row(value):
    depth = lax.axis_size("seq_2")
    count = lax.axis_size(SEQ)
    return lax.ppermute(
        value, SEQ, [(s, s + depth) for s in range(depth - 1, count - depth, depth)]
    )


def swap(value, axis):
    return lax.ppermute(value, axis, [(0, 1), (1, 0)])


def for_each(value, axis):
    size = lax.axis_size(axis)
    return lax.all_to_all(
        jnp.broadcast_to(value[None], (size, *value.shape)), axis, 0, 0, tiled=True
    )


def dot(a, b, dims):
    return lax.dot_general(a, b, (dims, ((), ())), preferred_element_type=F32)


NT = ((1,), (1,))
NN = ((1,), (0,))
TN = ((0,), (0,))


def squashed(k, q):
    t = jnp.tanh(dot(k, q, NT) * (SCALE / CAP))
    return t, jnp.exp2(t * EXP_MUL)


def places():
    shape = (TOK_DEV, GROUP * TOK_DEV)
    key = lax.broadcasted_iota(jnp.int32, shape, 0)
    query = lax.broadcasted_iota(jnp.int32, shape, 1) & (TOK_DEV - 1)
    return key, query


def two_heads(q_ref):
    return jnp.concatenate([q_ref[:, h * HEAD_DIM : (h + 1) * HEAD_DIM] for h in range(GROUP)], 0)


def row_sum(e):
    return jnp.sum(e, axis=0, keepdims=True)


def near_kernel(
    at_ref, q_ref, k0_ref, v0_ref, k1_ref, v1_ref, p_ref, pf_ref, acc_ref, tot_ref
):
    q = two_heads(q_ref)
    key, query = places()
    t, e = squashed(k1_ref[...], q)
    e = e * jnp.where(at_ref[0] >= 1, 1.0, 0.0)
    p1 = e.astype(BF16)
    p_ref[0, :TOK_DEV] = p1
    pf_ref[0, :TOK_DEV] = (e * (1.0 - t * t)).astype(BF16)
    total = row_sum(e)
    t, e = squashed(k0_ref[...], q)
    e = jnp.where(key <= query, e, 0.0)
    p0 = e.astype(BF16)
    p_ref[0, TOK_DEV:] = p0
    pf_ref[0, TOK_DEV:] = (e * (1.0 - t * t)).astype(BF16)
    total = total + row_sum(e)
    acc_ref[0] = dot(v1_ref[...], p1, TN) + dot(v0_ref[...], p0, TN)
    tot_ref[0] = jnp.broadcast_to(total, tot_ref.shape[1:])


def far_kernel(
    at_ref, q_ref, k2_ref, v2_ref, acc_ref, tot_ref,
    p_ref, pf_ref, attn_ref, inv_ref, out0_ref, out1_ref, out2_ref, out3_ref,
):
    key, query = places()
    t, e = squashed(k2_ref[...], two_heads(q_ref))
    e = jnp.where(key > query + jnp.where(at_ref[0] >= 2, 0, 4 * TOK_DEV), e, 0.0)
    p = e.astype(BF16)
    p_ref[0] = p
    pf_ref[0] = (e * (1.0 - t * t)).astype(BF16)
    inverse = 1.0 / (tot_ref[0, :1] + row_sum(e))
    inv_ref[0] = jnp.broadcast_to(inverse, inv_ref.shape[1:])
    out = ((acc_ref[0] + dot(v2_ref[...], p, TN)) * inverse).astype(BF16)
    out = jnp.concatenate([out[:, h * TOK_DEV : (h + 1) * TOK_DEV] for h in range(GROUP)], 0)
    attn_ref[0] = out
    place = (pl.program_id(0) + 4 - at_ref[1]) % 4
    for away, out_ref in enumerate((out0_ref, out1_ref, out2_ref, out3_ref)):

        @pl.when(place == away)
        def _():
            out_ref[...] = out


def score_terms(v, g, delta, pf):
    return (pf.astype(F32) * (dot(v, g, NN) - delta)).astype(BF16)


def far_grad_kernel(
    at_ref, scale_ref, q_ref, v2_ref, p_ref, pf_ref, inv_ref, attn_ref, m_own_ref, m_oth_ref,
    wa_ref, wc_ref, wbl_ref, wbh_ref, wdl_ref, wdh_ref,
    d2_ref, g_ref, delta_ref, ds_ref, raw_ref,
):
    act_scale = scale_ref[0]
    own = pl.multiple_of(at_ref[2] * TOK_DEV, TOK_DEV)
    oth = pl.multiple_of((1 - at_ref[2]) * TOK_DEV, TOK_DEV)
    both = dot(
        jnp.concatenate([wa_ref[0], wbl_ref[0], wbh_ref[0]], 0), m_own_ref[...], NT
    ) + dot(jnp.concatenate([wc_ref[0], wdl_ref[0], wdh_ref[0]], 0), m_oth_ref[...], NT)
    raw_ref[:, pl.ds(own, TOK_DEV)] = both[:HEAD_DIM]
    raw_ref[:, pl.ds(oth, TOK_DEV)] = both[HEAD_DIM:]
    g = (raw_ref[...] * inv_ref[0, :1]).astype(BF16)
    g_ref[0] = g
    attn = jnp.concatenate(
        [attn_ref[0, h * HEAD_DIM : (h + 1) * HEAD_DIM, :] for h in range(GROUP)], 1
    )
    delta = row_sum(g.astype(F32) * attn.astype(F32))
    delta_ref[0] = jnp.broadcast_to(delta, delta_ref.shape[1:])
    dscore = score_terms(v2_ref[...], g, delta, pf_ref[0])
    ds_ref[0] = dscore
    d2_ref[:TOK_DEV] = (dot(dscore, two_heads(q_ref), NN) * (SCALE * act_scale)).astype(BF16)
    d2_ref[TOK_DEV:] = (dot(p_ref[0], g, NT) * act_scale).astype(BF16)


def near_grad_kernel(
    scale_ref, q_ref, k0_ref, v0_ref, k1_ref, v1_ref, k2_ref, p_ref, pf_ref, g_ref, delta_ref, ds_ref,
    dq_ref, d0_ref, d1_ref, sq_ref,
):
    act_scale = scale_ref[0]
    q = two_heads(q_ref)
    g = g_ref[0]
    delta = delta_ref[0, :1]
    dq = dot(k2_ref[...], ds_ref[0], TN)
    for k, v, at, out in (
        (k1_ref[...], v1_ref[...], 0, d1_ref),
        (k0_ref[...], v0_ref[...], TOK_DEV, d0_ref),
    ):
        dscore = score_terms(v, g, delta, pf_ref[0, at : at + TOK_DEV])
        dq = dq + dot(k, dscore, TN)
        out[:TOK_DEV] = (dot(dscore, q, NN) * (SCALE * act_scale)).astype(out.dtype)
        out[TOK_DEV:] = (dot(p_ref[0, at : at + TOK_DEV], g, NT) * act_scale).astype(out.dtype)
    dq = dq * (SCALE * act_scale)
    sq_ref[...] = jnp.broadcast_to(jnp.sum(dq * dq), sq_ref.shape)
    for h in range(GROUP):
        dq_ref[:, h * HEAD_DIM : (h + 1) * HEAD_DIM] = dq[
            :, h * TOK_DEV : (h + 1) * TOK_DEV
        ].T.astype(BF16)


def weight_kernel(at_ref, a_own_ref, a_oth_ref, m0_ref, m1_ref, m2_ref, m3_ref, out_ref):
    acc = None
    for back, m_ref in enumerate((m0_ref, m1_ref, m2_ref, m3_ref)):
        both = dot(a_own_ref[back], m_ref[:TOK_DEV], NN) + dot(
            a_oth_ref[back], m_ref[TOK_DEV:], NN
        )
        acc = both if acc is None else acc + both
    acc = acc.reshape(2, 8, 2, 16, HALF)
    for low in range(2):
        for high in range(2):
            away = (2 * high + low + 4 - at_ref[3]) % 4
            out_ref[away] = acc[low, :, high].reshape(128, HALF).astype(BF16)


D = HEAD_DIM
SCORES = GROUP * TOK_DEV
HEAD_COLS = pl.BlockSpec((TOK_DEV, GROUP * D), lambda h, *_: (0, h))
KV_COLS = pl.BlockSpec((TOK_DEV, D), lambda h, *_: (0, h))
BOTH_COLS = pl.BlockSpec((2 * TOK_DEV, D), lambda h, *_: (0, h))
ATTN_ROWS = pl.BlockSpec((1, GROUP * D, TOK_DEV), lambda h, *_: (h, 0, 0))


def of_head(rows, columns=SCORES):
    return pl.BlockSpec((1, rows, columns), lambda h, *_: (h, 0, 0))


def per_head(rows, dtype):
    return jax.ShapeDtypeStruct((KV_HEADS, rows, SCORES), dtype)


def flat(rows, dtype):
    return jax.ShapeDtypeStruct((rows, KV_HEADS * D), dtype)


def call(kernel, scalars, in_specs, out_specs, out_shape, products, mib, scratch=()):
    return pl.pallas_call(
        kernel,
        grid_spec=pltpu.PrefetchScalarGridSpec(
            num_scalar_prefetch=scalars,
            grid=(KV_HEADS,),
            in_specs=in_specs,
            out_specs=out_specs,
            scratch_shapes=scratch,
        ),
        out_shape=out_shape,
        cost_estimate=pl.CostEstimate(
            flops=products * 2 * HEADS * TOK_DEV**3, transcendentals=0, bytes_accessed=mib << 20
        ),
    )


def near_forward(where, q, k, v, k1, v1):
    return call(
        near_kernel, 1,
        [HEAD_COLS] + [KV_COLS] * 4,
        [of_head(2 * TOK_DEV), of_head(2 * TOK_DEV), of_head(D), of_head(8)],
        [per_head(2 * TOK_DEV, BF16), per_head(2 * TOK_DEV, BF16), per_head(D, F32),
         per_head(8, F32)],
        4, 9,
    )(where, q, k, v, k1, v1)


def far_forward(where, q, k2, v2, acc, tot):
    return call(
        far_kernel, 1,
        [HEAD_COLS, KV_COLS, KV_COLS, of_head(D), of_head(8)],
        [of_head(TOK_DEV), of_head(TOK_DEV), ATTN_ROWS, of_head(8)]
        + [pl.BlockSpec((GROUP * D, TOK_DEV), lambda h, *_: (0, 0))] * 4,
        [per_head(TOK_DEV, BF16), per_head(TOK_DEV, BF16),
         jax.ShapeDtypeStruct((KV_HEADS, GROUP * D, TOK_DEV), BF16), per_head(8, F32)]
        + [jax.ShapeDtypeStruct((GROUP * D, TOK_DEV), BF16)] * 4,
        2, 7,
    )(where, q, k2, v2, acc, tot)


def far_backward(where, scale, q, v2, p, pf, inv, attn, m_own, m_oth, weights):
    full = pl.BlockSpec((TOK_DEV, HALF), lambda h, *_: (0, 0))
    rel = lambda rows: pl.BlockSpec((1, rows, HALF), lambda h, at, *_: ((at[1] + 4 - h) % 4, 0, 0))
    return call(
        far_grad_kernel, 2,
        [HEAD_COLS, KV_COLS, of_head(TOK_DEV), of_head(TOK_DEV), of_head(8), ATTN_ROWS, full,
         full, rel(D), rel(D)] + [rel(D // 2)] * 4,
        [BOTH_COLS, of_head(D), of_head(8), of_head(TOK_DEV)],
        [flat(2 * TOK_DEV, BF16), per_head(D, BF16), per_head(8, F32), per_head(TOK_DEV, BF16)],
        3 + 7, 15, [pltpu.VMEM((D, SCORES), F32)],
    )(where, scale, q, v2, p, pf, inv, attn, m_own, m_oth, *weights)


def near_backward(scale, q, k, v, k1, v1, k2, p, pf, g, delta, dscore):
    return call(
        near_grad_kernel, 1,
        [HEAD_COLS] + [KV_COLS] * 5
        + [of_head(2 * TOK_DEV), of_head(2 * TOK_DEV), of_head(D), of_head(8), of_head(TOK_DEV)],
        [HEAD_COLS, BOTH_COLS, BOTH_COLS, pl.BlockSpec((8, 128), lambda h, *_: (h, 0))],
        [jax.ShapeDtypeStruct((TOK_DEV, WIDTH), BF16), flat(2 * TOK_DEV, F32),
         flat(2 * TOK_DEV, BF16), jax.ShapeDtypeStruct((8 * KV_HEADS, 128), F32)],
        9, 13,
    )(scale, q, k, v, k1, v1, k2, p, pf, g, delta, dscore)


def weight_product(where, a_own, a_oth, m0, m1, m2, m3):
    vmem = pl.BlockSpec(memory_space=pltpu.VMEM)
    return pl.pallas_call(
        weight_kernel,
        in_specs=[pl.BlockSpec(memory_space=pltpu.SMEM)] + [vmem] * 6,
        out_specs=vmem,
        out_shape=jax.ShapeDtypeStruct((4, 128, HALF), BF16),
        cost_estimate=pl.CostEstimate(
            flops=2 * 512 * HALF * 2048, transcendentals=0, bytes_accessed=7 << 20
        ),
        name="weight_product",
    )(where, a_own, a_oth, m0, m1, m2, m3)


def all_steps(queries, keys, values, out_grad, out_weight, seq_len):
    q_rows = queries[0]
    k_rows = keys[0]
    v_rows = values[0]
    length = seq_len[0]
    core = lax.axis_index("dp_1")
    x_hi = lax.axis_index("dp_0")
    x_lo = lax.axis_index("seq_1")
    index = lax.axis_index(SEQ)
    start = index * TOK_DEV
    where = jnp.stack([index, lax.axis_index("seq_0"), x_lo, 2 * x_hi + x_lo]).astype(jnp.int32)

    at_end = lax.axis_index("seq_2") == lax.axis_size("seq_2") - 1
    h1k = shifted(k_rows, 1)
    h1v = jnp.where(at_end, next_row(v_rows), v_rows)
    h1v = ring(h1v, "seq_2", 1)
    h2k = shifted(h1k, 1)
    h2v = jnp.where(at_end, next_row(h1v), h1v)
    h2v = ring(h2v, "seq_2", 1)

    slots = TOK_DEV * lax.axis_size(SEQ) * lax.axis_size(DP)
    count = jnp.clip(length, 0, TOK_DEV * lax.axis_size(SEQ)).astype(F32).reshape(1)
    count = count + swap(count, "dp_1")
    count = count + swap(count, "dp_0")
    act_scale = slots / count
    weight_scale = lax.rsqrt(count[0])

    half_of = lambda a, c: lax.dynamic_slice_in_dim(a, c * HALF, HALF, 1)
    valid = (start + jnp.arange(TOK_DEV, dtype=jnp.int32)) < length
    masked = jnp.where(valid[:, None], out_grad[0], jnp.zeros((), BF16))
    m_own = half_of(masked, core)
    m_oth = half_of(masked, 1 - core)
    m0 = jnp.concatenate([m_own, swap(m_oth, "dp_1")], 0)
    m1 = ring(m0, "seq_0", 1)
    m3 = ring(m0, "seq_0", -1)
    m2 = ring(m3, "seq_0", -1)

    w_z = for_each(half_of(out_weight, core), "seq_2").reshape(HEAD_DIM, HALF)
    w_up = ring(w_z, "seq_0", 1)
    w_down = ring(w_z, "seq_0", -1)
    mid = HEAD_DIM // 2
    w_far = [ring(w_up[:mid], "seq_0", 1), ring(w_down[mid:], "seq_0", -1)]
    wa = jnp.stack([w_z, w_up, jnp.concatenate(w_far, 0), w_down])
    wbl = ring_x(wa[:, :mid], 1)
    wbh = ring_x(wa[:, mid:], -1)
    wc = swap(wa, "dp_1")
    wdl = swap(wbl, "dp_1")
    wdh = swap(wbh, "dp_1")

    p, pf, acc, tot = near_forward(where, q_rows, k_rows, v_rows, h1k, h1v)
    p2, pf2, attn, inv, *away = far_forward(where, q_rows, h2k, h2v, acc, tot)
    attn_parts = (
        away[0], ring(away[1], "seq_0", 1), ring(away[2], "seq_0", 2), ring(away[3], "seq_0", -1)
    )

    d2, g, delta, dscore = far_backward(
        where, act_scale, q_rows, h2v, p2, pf2, inv, attn, m_own, m_oth,
        (wa, wc, wbl, wbh, wdl, wdh),
    )
    attn_parts, _ = lax.optimization_barrier((attn_parts, delta))
    a_own = jnp.stack(attn_parts)
    a_oth = swap(a_own, "dp_1")

    r1 = shifted(d2, -1)
    dq, d0, d1, dq_sq = near_backward(
        act_scale, q_rows, k_rows, v_rows, h1k, h1v, h2k, p, pf, g, delta, dscore
    )
    part = weight_product(
        where, a_own, a_oth, m0, m1, m2, m3
    )
    r1, _ = lax.optimization_barrier((r1, part))
    r2 = shifted((d1.astype(F32) + r1.astype(F32)).astype(BF16), -1)
    dkv = d0 + r2.astype(F32)
    square = jnp.sum(dkv * dkv)
    square = square + jnp.sum(dq_sq.reshape(KV_HEADS, 8, 128)[:, 0, 0])
    dkv = dkv.astype(BF16)

    part = (
        part[0].astype(F32)
        + ring_x(part[1], 1).astype(F32)
        + ring_x(part[2], 2).astype(F32)
        + ring_x(part[3], -1).astype(F32)
    ).astype(BF16)
    pieces = lax.all_to_all(part, "seq_2", 0, 0, tiled=True)
    piece = jnp.sum(pieces.reshape(8, 16, HALF).astype(F32), axis=0) * weight_scale
    square = square + jnp.sum(piece * piece)

    other = swap(piece, "dp_1")
    row = jnp.where(
        core == 0, jnp.concatenate([piece, other], 1), jnp.concatenate([other, piece], 1)
    )
    other = swap(row, "dp_0")
    weight_grad = jnp.where(
        x_hi == 0, jnp.concatenate([row, other], 0), jnp.concatenate([other, row], 0)
    )

    square = jnp.full((8, 128), square, F32)
    square = for_each(square, ("dp_0", "seq_1", "dp_1"))
    square = jnp.full((8, 128), jnp.sum(square[:, 0], axis=0)[0], F32)
    square = for_each(square, ("seq_0", "seq_2"))
    square = jnp.sum(square[:, 0], axis=0)[0]
    entries = slots * (HEADS + 2 * KV_HEADS) * HEAD_DIM + WIDTH * D_OUT
    grad_rms = jnp.sqrt(square / entries)
    return (dq[None], dkv[:TOK_DEV][None], dkv[TOK_DEV:][None], weight_grad, grad_rms)


def solution(mesh):
    split = Mesh(mesh.devices.reshape(4, 2, 8, 2, 2), ("seq_0", "seq_1", "seq_2", "dp_0", "dp_1"))
    placed = (
        P(DP, SEQ, None),
        P(DP, SEQ, None),
        P(DP, SEQ, None),
        P(DP, SEQ, None),
        P(SEQ, None),
        P(DP),
    )
    return jax.shard_map(
        all_steps,
        mesh=split,
        in_specs=placed,
        out_specs=(P(DP, SEQ, None), P(DP, SEQ, None), P(DP, SEQ, None), P(SEQ, None), P()),
        check_vma=False,
    )
```

```python
import math

import jax
import jax.numpy as jnp
from jax import lax
from jax.experimental import pallas as pl
from jax.experimental.pallas import tpu as pltpu
from jax.sharding import Mesh
from jax.sharding import PartitionSpec as P


HEADS = 8
KV_HEADS = 4
GROUP = HEADS // KV_HEADS
HEAD_DIM = 256
D_OUT = 1792
HALF = D_OUT // 2
TOK_DEV = 256
WIDTH = HEADS * HEAD_DIM
SEQ = ("seq_0", "seq_1", "seq_2")
DP = ("dp_0", "dp_1")
X_AXES = ("seq_1", "dp_0")
SCALE = 0.0625
CAP = 50.0
EXP_MUL = CAP * math.log2(math.e)
BF16 = jnp.bfloat16
F32 = jnp.float32


def shifted(value, steps):
    count = lax.axis_size(SEQ)
    initial, last = (max(0, -steps), min(count, count - steps))
    return lax.ppermute(value, SEQ, [(source, source + steps) for source in range(initial, last)])


def ring(value, axis, steps):
    count = lax.axis_size(axis)
    return lax.ppermute(value, axis, [(s, (s + steps) % count) for s in range(count)])


def ring_x(value, steps):
    at = lambda x: (x % 2) * 2 + x // 2
    return lax.ppermute(value, X_AXES, [(at(s), at((s + steps) % 4)) for s in range(4)])


def next_row(value):
    depth = lax.axis_size("seq_2")
    count = lax.axis_size(SEQ)
    return lax.ppermute(
        value, SEQ, [(s, s + depth) for s in range(depth - 1, count - depth, depth)]
    )


def swap(value, axis):
    return lax.ppermute(value, axis, [(0, 1), (1, 0)])


def for_each(value, axis):
    size = lax.axis_size(axis)
    return lax.all_to_all(
        jnp.broadcast_to(value[None], (size, *value.shape)), axis, 0, 0, tiled=True
    )


def dot(a, b, dims):
    return lax.dot_general(a, b, (dims, ((), ())), preferred_element_type=F32)


NT = ((1,), (1,))
NN = ((1,), (0,))
TN = ((0,), (0,))


def squashed(k, q):
    t = jnp.tanh(dot(k, q, NT) * (SCALE / CAP))
    return t, jnp.exp2(t * EXP_MUL)


def places():
    shape = (TOK_DEV, GROUP * TOK_DEV)
    key = lax.broadcasted_iota(jnp.int32, shape, 0)
    query = lax.broadcasted_iota(jnp.int32, shape, 1) & (TOK_DEV - 1)
    return key, query


def two_heads(q_ref):
    return jnp.concatenate([q_ref[:, h * HEAD_DIM : (h + 1) * HEAD_DIM] for h in range(GROUP)], 0)


def row_sum(e):
    return jnp.sum(e, axis=0, keepdims=True)


def near_kernel(
    at_ref, q_ref, k0_ref, v0_ref, k1_ref, v1_ref, p_ref, pf_ref, acc_ref, tot_ref
):
    q = two_heads(q_ref)
    key, query = places()
    t, e = squashed(k1_ref[...], q)
    e = e * jnp.where(at_ref[0] >= 1, 1.0, 0.0)
    p1 = e.astype(BF16)
    p_ref[0, :TOK_DEV] = p1
    pf_ref[0, :TOK_DEV] = (e * (1.0 - t * t)).astype(BF16)
    total = row_sum(e)
    t, e = squashed(k0_ref[...], q)
    e = jnp.where(key <= query, e, 0.0)
    p0 = e.astype(BF16)
    p_ref[0, TOK_DEV:] = p0
    pf_ref[0, TOK_DEV:] = (e * (1.0 - t * t)).astype(BF16)
    total = total + row_sum(e)
    acc_ref[0] = dot(v1_ref[...], p1, TN) + dot(v0_ref[...], p0, TN)
    tot_ref[0] = jnp.broadcast_to(total, tot_ref.shape[1:])


def far_kernel(
    at_ref, q_ref, k2_ref, v2_ref, acc_ref, tot_ref,
    p_ref, pf_ref, attn_ref, inv_ref, out0_ref, out1_ref, out2_ref, out3_ref,
):
    key, query = places()
    t, e = squashed(k2_ref[...], two_heads(q_ref))
    e = jnp.where(key > query + jnp.where(at_ref[0] >= 2, 0, 4 * TOK_DEV), e, 0.0)
    p = e.astype(BF16)
    p_ref[0] = p
    pf_ref[0] = (e * (1.0 - t * t)).astype(BF16)
    inverse = 1.0 / (tot_ref[0, :1] + row_sum(e))
    inv_ref[0] = jnp.broadcast_to(inverse, inv_ref.shape[1:])
    out = ((acc_ref[0] + dot(v2_ref[...], p, TN)) * inverse).astype(BF16)
    out = jnp.concatenate([out[:, h * TOK_DEV : (h + 1) * TOK_DEV] for h in range(GROUP)], 0)
    attn_ref[0] = out
    place = (pl.program_id(0) + 4 - at_ref[1]) % 4
    for away, out_ref in enumerate((out0_ref, out1_ref, out2_ref, out3_ref)):

        @pl.when(place == away)
        def _():
            out_ref[...] = out


def score_terms(v, g, delta, pf):
    return (pf.astype(F32) * (dot(v, g, NN) - delta)).astype(BF16)


def far_grad_kernel(
    at_ref, scale_ref, q_ref, v2_ref, p_ref, pf_ref, inv_ref, attn_ref, m_own_ref, m_oth_ref,
    wa_ref, wc_ref, wbl_ref, wbh_ref, wdl_ref, wdh_ref,
    d2_ref, g_ref, delta_ref, ds_ref, raw_ref,
):
    act_scale = scale_ref[0]
    own = pl.multiple_of(at_ref[2] * TOK_DEV, TOK_DEV)
    oth = pl.multiple_of((1 - at_ref[2]) * TOK_DEV, TOK_DEV)
    both = dot(
        jnp.concatenate([wa_ref[0], wbl_ref[0], wbh_ref[0]], 0), m_own_ref[...], NT
    ) + dot(jnp.concatenate([wc_ref[0], wdl_ref[0], wdh_ref[0]], 0), m_oth_ref[...], NT)
    raw_ref[:, pl.ds(own, TOK_DEV)] = both[:HEAD_DIM]
    raw_ref[:, pl.ds(oth, TOK_DEV)] = both[HEAD_DIM:]
    g = (raw_ref[...] * inv_ref[0, :1]).astype(BF16)
    g_ref[0] = g
    attn = jnp.concatenate(
        [attn_ref[0, h * HEAD_DIM : (h + 1) * HEAD_DIM, :] for h in range(GROUP)], 1
    )
    delta = row_sum(g.astype(F32) * attn.astype(F32))
    delta_ref[0] = jnp.broadcast_to(delta, delta_ref.shape[1:])
    dscore = score_terms(v2_ref[...], g, delta, pf_ref[0])
    ds_ref[0] = dscore
    d2_ref[:TOK_DEV] = (dot(dscore, two_heads(q_ref), NN) * (SCALE * act_scale)).astype(BF16)
    d2_ref[TOK_DEV:] = (dot(p_ref[0], g, NT) * act_scale).astype(BF16)


def mid_grad_kernel(
    scale_ref, q_ref, v1_ref, p_ref, pf_ref, g_ref, delta_ref, d1_ref, ds_ref,
):
    act_scale = scale_ref[0]
    g = g_ref[0]
    dscore = score_terms(v1_ref[...], g, delta_ref[0, :1], pf_ref[0])
    d1_ref[:TOK_DEV] = (dot(dscore, two_heads(q_ref), NN) * (SCALE * act_scale)).astype(BF16)
    d1_ref[TOK_DEV:] = (dot(p_ref[0], g, NT) * act_scale).astype(BF16)
    ds_ref[0] = dscore


def near_grad_kernel(
    scale_ref, q_ref, k0_ref, v0_ref, k1_ref, k2_ref, p_ref, pf_ref, g_ref, delta_ref, ds1_ref,
    ds2_ref, dq_ref, d0_ref, sq_ref,
):
    act_scale = scale_ref[0]
    g = g_ref[0]
    dscore = score_terms(v0_ref[...], g, delta_ref[0, :1], pf_ref[0])
    d0_ref[:TOK_DEV] = dot(dscore, two_heads(q_ref), NN) * (SCALE * act_scale)
    d0_ref[TOK_DEV:] = dot(p_ref[0], g, NT) * act_scale
    dq = (
        dot(k2_ref[...], ds2_ref[0], TN)
        + dot(k1_ref[...], ds1_ref[0], TN)
        + dot(k0_ref[...], dscore, TN)
    ) * (SCALE * act_scale)
    sq_ref[...] = jnp.broadcast_to(jnp.sum(dq * dq), sq_ref.shape)
    for h in range(GROUP):
        dq_ref[:, h * HEAD_DIM : (h + 1) * HEAD_DIM] = dq[
            :, h * TOK_DEV : (h + 1) * TOK_DEV
        ].T.astype(BF16)


def weight_kernel(at_ref, a_own_ref, a_oth_ref, m0_ref, m1_ref, m2_ref, m3_ref, *out_refs):
    acc = None
    for back, m_ref in enumerate((m0_ref, m1_ref, m2_ref, m3_ref)):
        both = dot(a_own_ref[back], m_ref[:TOK_DEV], NN) + dot(
            a_oth_ref[back], m_ref[TOK_DEV:], NN
        )
        acc = both if acc is None else acc + both
    acc = acc.reshape(2, 8, 2, 16, HALF)
    for low in range(2):
        for high in range(2):
            away = (2 * high + low + 4 - at_ref[3]) % 4
            rows = acc[low, :, high].reshape(128, HALF).astype(BF16)
            for place, out_ref in enumerate(out_refs):

                @pl.when(away == place)
                def _(out_ref=out_ref, rows=rows):
                    out_ref[...] = rows


D = HEAD_DIM
SCORES = GROUP * TOK_DEV
HEAD_COLS = pl.BlockSpec((TOK_DEV, GROUP * D), lambda h, *_: (0, h))
KV_COLS = pl.BlockSpec((TOK_DEV, D), lambda h, *_: (0, h))
BOTH_COLS = pl.BlockSpec((2 * TOK_DEV, D), lambda h, *_: (0, h))
ATTN_ROWS = pl.BlockSpec((1, GROUP * D, TOK_DEV), lambda h, *_: (h, 0, 0))


def of_head(rows, columns=SCORES):
    return pl.BlockSpec((1, rows, columns), lambda h, *_: (h, 0, 0))


def per_head(rows, dtype):
    return jax.ShapeDtypeStruct((KV_HEADS, rows, SCORES), dtype)


def flat(rows, dtype):
    return jax.ShapeDtypeStruct((rows, KV_HEADS * D), dtype)


def call(kernel, scalars, in_specs, out_specs, out_shape, products, mib, scratch=()):
    return pl.pallas_call(
        kernel,
        grid_spec=pltpu.PrefetchScalarGridSpec(
            num_scalar_prefetch=scalars,
            grid=(KV_HEADS,),
            in_specs=in_specs,
            out_specs=out_specs,
            scratch_shapes=scratch,
        ),
        out_shape=out_shape,
        cost_estimate=pl.CostEstimate(
            flops=products * 2 * HEADS * TOK_DEV**3, transcendentals=0, bytes_accessed=mib << 20
        ),
    )


def near_forward(where, q, k, v, k1, v1):
    return call(
        near_kernel, 1,
        [HEAD_COLS] + [KV_COLS] * 4,
        [of_head(2 * TOK_DEV), of_head(2 * TOK_DEV), of_head(D), of_head(8)],
        [per_head(2 * TOK_DEV, BF16), per_head(2 * TOK_DEV, BF16), per_head(D, F32),
         per_head(8, F32)],
        4, 9,
    )(where, q, k, v, k1, v1)


def far_forward(where, q, k2, v2, acc, tot):
    return call(
        far_kernel, 1,
        [HEAD_COLS, KV_COLS, KV_COLS, of_head(D), of_head(8)],
        [of_head(TOK_DEV), of_head(TOK_DEV), ATTN_ROWS, of_head(8)]
        + [pl.BlockSpec((GROUP * D, TOK_DEV), lambda h, *_: (0, 0))] * 4,
        [per_head(TOK_DEV, BF16), per_head(TOK_DEV, BF16),
         jax.ShapeDtypeStruct((KV_HEADS, GROUP * D, TOK_DEV), BF16), per_head(8, F32)]
        + [jax.ShapeDtypeStruct((GROUP * D, TOK_DEV), BF16)] * 4,
        2, 7,
    )(where, q, k2, v2, acc, tot)


def far_backward(where, scale, q, v2, p, pf, inv, attn, m_own, m_oth, weights):
    full = pl.BlockSpec((TOK_DEV, HALF), lambda h, *_: (0, 0))
    rel = lambda rows: pl.BlockSpec((1, rows, HALF), lambda h, at, *_: ((at[1] + 4 - h) % 4, 0, 0))
    return call(
        far_grad_kernel, 2,
        [HEAD_COLS, KV_COLS, of_head(TOK_DEV), of_head(TOK_DEV), of_head(8), ATTN_ROWS, full,
         full, rel(D), rel(D)] + [rel(D // 2)] * 4,
        [BOTH_COLS, of_head(D), of_head(8), of_head(TOK_DEV)],
        [flat(2 * TOK_DEV, BF16), per_head(D, BF16), per_head(8, F32), per_head(TOK_DEV, BF16)],
        3 + 7, 15, [pltpu.VMEM((D, SCORES), F32)],
    )(where, scale, q, v2, p, pf, inv, attn, m_own, m_oth, *weights)


def part_of_head(which):
    return pl.BlockSpec((1, TOK_DEV, SCORES), lambda h, *_: (h, which, 0))


def mid_backward(scale, q, v1, p, pf, g, delta):
    return call(
        mid_grad_kernel, 1,
        [HEAD_COLS, KV_COLS, part_of_head(0), part_of_head(0), of_head(D), of_head(8)],
        [BOTH_COLS, of_head(TOK_DEV)],
        [flat(2 * TOK_DEV, BF16), per_head(TOK_DEV, BF16)],
        3, 7,
    )(scale, q, v1, p, pf, g, delta)


def near_backward(scale, q, k, v, k1, k2, p, pf, g, delta, ds1, ds2):
    return call(
        near_grad_kernel, 1,
        [HEAD_COLS] + [KV_COLS] * 4
        + [part_of_head(1), part_of_head(1), of_head(D), of_head(8), of_head(TOK_DEV),
           of_head(TOK_DEV)],
        [HEAD_COLS, BOTH_COLS, pl.BlockSpec((8, 128), lambda h, *_: (h, 0))],
        [jax.ShapeDtypeStruct((TOK_DEV, WIDTH), BF16), flat(2 * TOK_DEV, F32),
         jax.ShapeDtypeStruct((8 * KV_HEADS, 128), F32)],
        5, 10,
    )(scale, q, k, v, k1, k2, p, pf, g, delta, ds1, ds2)


def weight_product(where, a_own, a_oth, m0, m1, m2, m3):
    vmem = pl.BlockSpec(memory_space=pltpu.VMEM)
    return pl.pallas_call(
        weight_kernel,
        in_specs=[pl.BlockSpec(memory_space=pltpu.SMEM)] + [vmem] * 6,
        out_specs=[vmem] * 4,
        out_shape=[jax.ShapeDtypeStruct((128, HALF), BF16)] * 4,
        cost_estimate=pl.CostEstimate(
            flops=2 * 512 * HALF * 2048, transcendentals=0, bytes_accessed=7 << 20
        ),
        name="weight_product",
    )(where, a_own, a_oth, m0, m1, m2, m3)


def all_steps(queries, keys, values, out_grad, out_weight, seq_len):
    q_rows = queries[0]
    k_rows = keys[0]
    v_rows = values[0]
    length = seq_len[0]
    core = lax.axis_index("dp_1")
    x_hi = lax.axis_index("dp_0")
    x_lo = lax.axis_index("seq_1")
    index = lax.axis_index(SEQ)
    start = index * TOK_DEV
    where = jnp.stack([index, lax.axis_index("seq_0"), x_lo, 2 * x_hi + x_lo]).astype(jnp.int32)

    at_end = lax.axis_index("seq_2") == lax.axis_size("seq_2") - 1
    h1k = shifted(k_rows, 1)
    h1v = jnp.where(at_end, next_row(v_rows), v_rows)
    h1v = ring(h1v, "seq_2", 1)
    h2k = shifted(h1k, 1)
    h2v = jnp.where(at_end, next_row(h1v), h1v)
    h2v = ring(h2v, "seq_2", 1)

    slots = TOK_DEV * lax.axis_size(SEQ) * lax.axis_size(DP)
    count = jnp.clip(length, 0, TOK_DEV * lax.axis_size(SEQ)).astype(F32).reshape(1)
    count = count + swap(count, "dp_1")
    count = count + swap(count, "dp_0")
    act_scale = slots / count
    weight_scale = lax.rsqrt(count[0])

    half_of = lambda a, c: lax.dynamic_slice_in_dim(a, c * HALF, HALF, 1)
    valid = (start + jnp.arange(TOK_DEV, dtype=jnp.int32)) < length
    masked = jnp.where(valid[:, None], out_grad[0], jnp.zeros((), BF16))
    m_own = half_of(masked, core)
    m_oth = half_of(masked, 1 - core)
    m0 = jnp.concatenate([m_own, swap(m_oth, "dp_1")], 0)
    m1 = ring(m0, "seq_0", 1)
    m3 = ring(m0, "seq_0", -1)
    m2 = ring(m3, "seq_0", -1)

    w_z = for_each(half_of(out_weight, core), "seq_2").reshape(HEAD_DIM, HALF)
    w_up = ring(w_z, "seq_0", 1)
    w_down = ring(w_z, "seq_0", -1)
    mid = HEAD_DIM // 2
    w_far = [ring(w_up[:mid], "seq_0", 1), ring(w_down[mid:], "seq_0", -1)]
    wa = jnp.stack([w_z, w_up, jnp.concatenate(w_far, 0), w_down])
    wbl = ring_x(wa[:, :mid], 1)
    wbh = ring_x(wa[:, mid:], -1)
    wc = swap(wa, "dp_1")
    wdl = swap(wbl, "dp_1")
    wdh = swap(wbh, "dp_1")

    p, pf, acc, tot = near_forward(where, q_rows, k_rows, v_rows, h1k, h1v)
    p2, pf2, attn, inv, *away = far_forward(where, q_rows, h2k, h2v, acc, tot)
    attn_parts = (
        away[0], ring(away[1], "seq_0", 1), ring(away[2], "seq_0", 2), ring(away[3], "seq_0", -1)
    )

    d2, g, delta, dscore = far_backward(
        where, act_scale, q_rows, h2v, p2, pf2, inv, attn, m_own, m_oth,
        (wa, wc, wbl, wbh, wdl, wdh),
    )
    attn_parts, _ = lax.optimization_barrier((attn_parts, delta))
    a_own = jnp.stack(attn_parts)
    a_oth = swap(a_own, "dp_1")

    r1 = shifted(d2, -1)
    d1, dscore1 = mid_backward(act_scale, q_rows, h1v, p, pf, g, delta)
    dq, d0, dq_sq = near_backward(
        act_scale, q_rows, k_rows, v_rows, h1k, h2k, p, pf, g, delta, dscore1, dscore
    )
    part = weight_product(
        where, a_own, a_oth, m0, m1, m2, m3
    )
    r1, _ = lax.optimization_barrier((r1, part))
    r2 = shifted((d1.astype(F32) + r1.astype(F32)).astype(BF16), -1)
    dkv = d0 + r2.astype(F32)
    square = jnp.sum(dkv * dkv)
    square = square + jnp.sum(dq_sq.reshape(KV_HEADS, 8, 128)[:, 0, 0])
    dkv = dkv.astype(BF16)

    part = (
        part[0].astype(F32)
        + ring_x(part[1], 1).astype(F32)
        + ring_x(part[2], 2).astype(F32)
        + ring_x(part[3], -1).astype(F32)
    ).astype(BF16)
    pieces = lax.all_to_all(part, "seq_2", 0, 0, tiled=True)
    piece = jnp.sum(pieces.reshape(8, 16, HALF).astype(F32), axis=0) * weight_scale
    piece_square = jnp.sum(piece * piece)
    square = square + piece_square

    other = swap(piece, "dp_1")
    row = jnp.where(
        core == 0, jnp.concatenate([piece, other], 1), jnp.concatenate([other, piece], 1)
    )
    other = swap(row, "dp_0")
    weight_grad = jnp.where(
        x_hi == 0, jnp.concatenate([row, other], 0), jnp.concatenate([other, row], 0)
    )

    square = jnp.full((8, 128), square, F32)
    square = for_each(square, ("dp_0", "seq_1", "dp_1"))
    square = jnp.full((8, 128), jnp.sum(square[:, 0], axis=0)[0], F32)
    square = for_each(square, ("seq_0", "seq_2"))
    square = jnp.sum(square[:, 0], axis=0)[0]
    entries = slots * (HEADS + 2 * KV_HEADS) * HEAD_DIM + WIDTH * D_OUT
    grad_rms = jnp.sqrt(square / entries)
    return (dq[None], dkv[:TOK_DEV][None], dkv[TOK_DEV:][None], weight_grad, grad_rms)


def solution(mesh):
    split = Mesh(mesh.devices.reshape(4, 2, 8, 2, 2), ("seq_0", "seq_1", "seq_2", "dp_0", "dp_1"))
    placed = (
        P(DP, SEQ, None),
        P(DP, SEQ, None),
        P(DP, SEQ, None),
        P(DP, SEQ, None),
        P(SEQ, None),
        P(DP),
    )
    return jax.shard_map(
        all_steps,
        mesh=split,
        in_specs=placed,
        out_specs=(P(DP, SEQ, None), P(DP, SEQ, None), P(DP, SEQ, None), P(SEQ, None), P()),
        check_vma=False,
    )
```
